256 devices in a mesh: row: 16 (over x, z_hi), col: 16 (over y, z_lo, core).
Axes of the slice: x: 4, y: 4, z: 8 (z_hi: 4, z_lo: 2; z = z_hi * 2 + z_lo), core: 2. Of those that a mesh axis runs over, the one named last changes fastest.
Arguments:
- tokens: bfloat16 [2048, 8192], P('col', 'row'), may hold values from -6 to 6
- grad_out: bfloat16 [2048, 8192], P('col', 'row'), may hold values from -2 to 2
- gate: bfloat16 [2048, 14336], P('row', 'col'), may hold values from -6 to 6
- up: bfloat16 [2048, 14336], P('row', 'col'), may hold values from -6 to 6
- gate_weight: bfloat16 [8192, 14336], P('row', 'col'), may hold values from -0.0625 to 0.0625
- up_weight: bfloat16 [8192, 14336], P('row', 'col'), may hold values from -0.0625 to 0.0625
- down_weight: bfloat16 [8192, 14336], P('row', 'col'), may hold values from -0.046875 to 0.046875
Outputs:
- grad_tokens: bfloat16 [2048, 8192], P('col', 'row')
- grad_gate_weight: float32 [8192, 14336], P('row', 'col')
- grad_up_weight: float32 [8192, 14336], P('row', 'col')
- grad_down_weight: float32 [8192, 14336], P('row', 'col')
The draws below stay inside these ranges and needn't reach their ends.
All inputs are finite; a program needn't handle non-finite values.
Results may differ from the reference program's by a relative error of at most 0.0049.
Values may be sent and summed in bfloat16 or wider, within the bound.
A program may use at most 128 MiB of HBM per device.

```python
import jax
import jax.numpy as jnp
from jax import lax

D = 8192
FF = 14336
TOKENS = 2048


def raised(result, key, source, target, blocks, factor):
    def block_of(dim):
        return (jnp.arange(result.shape[dim]) // (result.shape[dim] // blocks)).reshape((-1,) + (1,) * (result.ndim - 1 - dim))

    near = jax.random.permutation(key, blocks)[block_of(target)]
    second = (block_of(target) + blocks // 2) % blocks
    return jnp.where((block_of(source) == near) | (block_of(source) == second), factor * result, result)


def block_scale(own_key, shape, pieces, low, high):
    def one(dim, parts):
        draws = jax.random.uniform(jax.random.fold_in(jax.random.fold_in(own_key, 6), dim), (parts,), jnp.float32, low / len(pieces), high / len(pieces))
        return jnp.repeat(jnp.exp(draws), shape[dim] // parts).reshape((-1,) + (1,) * (len(shape) - dim - 1))

    level = one(*pieces[0])
    for cut in pieces[1:]:
        level = level * one(*cut)
    return level


def noise(key, shape, scale, bound, split=(), kind=jnp.bfloat16):
    result = scale * jax.random.normal(key, shape, jnp.float32)
    if split:
        result = result * block_scale(key, shape, split, -0.22, 0.18)
    return jnp.clip(result, -bound, bound).astype(kind)


def bell_draw_with(rng, shape, scale, most, shards, heavy, held_as=jnp.bfloat16):
    array = scale * jax.random.normal(rng, shape, jnp.float32)
    if shards:
        array = array * block_scale(rng, shape, shards, -0.22, 0.18)
    return jnp.clip(raised(array, jax.random.fold_in(rng, 3), *heavy), -most, most).astype(held_as)


def setup_inputs(seed: int = 0) -> dict:
    splits = jax.random.split(jax.random.key(seed), 8)
    tokens = noise(splits[0], (TOKENS, D), 1.0, 6.0, ((0, 16), (1, 16)))
    grad_out = bell_draw_with(splits[1], (TOKENS, D), 0.25, 2.0, ((0, 16), (1, 16)), (1, 0, 16, 2.0))
    gate = noise(splits[2], (TOKENS, FF), 1.0, 6.0, ((0, 16), (1, 16)))
    up = noise(splits[3], (TOKENS, FF), 1.0, 6.0, ((0, 16), (1, 16)))
    gate_weight = noise(splits[4], (D, FF), D ** -0.5, 0.0625, ((0, 16), (1, 16)))
    up_weight = noise(splits[5], (D, FF), D ** -0.5, 0.0625, ((0, 16), (1, 16)))
    down_weight = noise(splits[6], (D, FF), FF ** -0.5, 0.046875, ((0, 16), (1, 16)))
    return {"tokens": tokens, "grad_out": grad_out, "gate": gate, "up": up, "gate_weight": gate_weight, "up_weight": up_weight, "down_weight": down_weight}


def reference(tokens, grad_out, gate, up, gate_weight, up_weight, down_weight):
    gate32 = gate.astype(jnp.float32)
    up32 = up.astype(jnp.float32)
    sigma = jax.nn.sigmoid(gate32)
    active = gate32 * sigma
    hidden = (active * up32).astype(jnp.bfloat16)
    grad_hidden = jnp.dot(grad_out, down_weight, preferred_element_type=jnp.float32)
    grad_up = (grad_hidden * active).astype(jnp.bfloat16)
    grad_gate = (grad_hidden * up32 * sigma * (1.0 + gate32 * (1.0 - sigma))).astype(jnp.bfloat16)
    grad_down_weight = jnp.dot(grad_out.T, hidden, preferred_element_type=jnp.float32)
    grad_gate_weight = jnp.dot(tokens.T, grad_gate, preferred_element_type=jnp.float32)
    grad_up_weight = jnp.dot(tokens.T, grad_up, preferred_element_type=jnp.float32)
    dims = (((1,), (1,)), ((), ()))
    grad_tokens = lax.dot_general(grad_gate, gate_weight, dims, preferred_element_type=jnp.float32)
    grad_tokens = grad_tokens + lax.dot_general(grad_up, up_weight, dims, preferred_element_type=jnp.float32)
    return grad_tokens.astype(jnp.bfloat16), grad_gate_weight, grad_up_weight, grad_down_weight
```

```python
import jax
import jax.numpy as jnp
from jax import lax
from jax.experimental import pallas as pl
from jax.experimental.pallas import tpu as pltpu
from jax.sharding import PartitionSpec as P

MESH = pl.DeviceIdType.MESH
BF = jnp.bfloat16
F32 = jnp.float32
B = 128
H = B // 2
N_MSG = 176


def rows(ref, start, size):
    return ref.at[pl.ds(pl.multiple_of(start, H), size), :]


class Net:
    def __init__(self, send, recv, me):
        self.send_sem, self.recv_sem, self.me = send, recv, me
        self.count = 0
        self.sent = []

    def take(self, n):
        first = self.count
        self.count += n
        return first

    def copy(self, src, dst, msg, device):
        return pltpu.make_async_remote_copy(
            src_ref=src, dst_ref=dst, send_sem=self.send_sem.at[msg], recv_sem=self.recv_sem.at[msg],
            device_id=device, device_id_type=MESH,
        )

    def send(self, src, dst, msg, device):
        copy = self.copy(src, dst, msg, device)
        copy.start()
        self.sent.append(copy)

    def recv(self, dst, msg):
        self.copy(dst, dst, msg, self.me).wait_recv()

    def drain(self):
        for copy in self.sent:
            copy.wait_send()


class Ring:
    def __init__(self, net, buf, pos, device_of, slot_of):
        self.net, self.buf, self.pos, self.device_of, self.slot_of = net, buf, pos, device_of, slot_of
        self.right, self.far, self.left = (lax.rem(pos + n, 4) for n in (1, 2, 3))
        self.msg = net.take(4)

    def start(self, src=None):
        own = rows(self.buf, self.slot_of(self.pos), B)
        src = own if src is None else src
        self.net.send(src, own, self.msg, self.device_of(self.right))
        self.net.send(src, own, self.msg + 1, self.device_of(self.left))

    def from_left(self):
        slot = self.slot_of(self.left)
        self.net.recv(rows(self.buf, slot, B), self.msg)
        half = rows(self.buf, slot, H)
        self.net.send(half, half, self.msg + 2, self.device_of(self.right))

    def from_right(self):
        slot = self.slot_of(self.right)
        self.net.recv(rows(self.buf, slot, B), self.msg + 1)
        half = rows(self.buf, slot + H, H)
        self.net.send(half, half, self.msg + 3, self.device_of(self.left))

    def neighbours(self):
        self.from_left()
        self.from_right()

    def from_far(self):
        slot = self.slot_of(self.far)
        self.net.recv(rows(self.buf, slot, H), self.msg + 2)
        self.net.recv(rows(self.buf, slot + H, H), self.msg + 3)


def dot(a, b, dims):
    return lax.dot_general(a, b, (dims, ((), ())), preferred_element_type=F32)


def kernel(
    tok, go, gate, up, gw, uw, dw,
    gt_out, dgw, duw, ddw,
    go_all, tok_all, hid, gg, gu, part, s1, s2r, s2l, r1l, r1r, r2l, r2r,
    xs, zs1, zs2r, zs2l, zr1l, zr1r, zr2l, zr2r,
    gt_own, d2d_s, d2d_r, gt_s, gt_r, gt_acc,
    send_sem, recv_sem,
):
    row, col = lax.axis_index("row"), lax.axis_index("col")
    x, zh = lax.div(row, 4), lax.rem(row, 4)
    y, zl, k = lax.div(col, 4), lax.rem(lax.div(col, 2), 2), lax.rem(col, 2)
    net = Net(send_sem, recv_sem, (row, col))
    other = 1 - zl

    def x_dev(p):
        return (p * 4 + zh, col)

    def z_dev(p):
        return (x * 4 + p, col)

    def y_dev(p):
        return (row, p * 4 + zl * 2 + k)

    partner = (row, y * 4 + zl * 2 + 1 - k)
    across = (row, y * 4 + other * 2 + k)
    xr, xf, xl = (lax.rem(x + n, 4) for n in (1, 2, 3))
    zr, zf, zlft = (lax.rem(zh + n, 4) for n in (1, 2, 3))

    barrier = pltpu.get_barrier_semaphore()
    peers = [x_dev(xr), x_dev(xl), z_dev(zr), z_dev(zlft), partner, across]
    for dy in (1, 2, 3):
        p = lax.rem(y + dy, 4)
        peers += [(row, p * 4 + zl * 2 + k), (row, p * 4 + other * 2 + k)]
    for peer in peers:
        pl.semaphore_signal(barrier, inc=1, device_id=peer, device_id_type=MESH)
    pl.semaphore_wait(barrier, len(peers))

    class Column:
        def __init__(self, own, buf):
            self.own, self.buf = own, buf
            self.y0 = Ring(net, buf, y, y_dev, lambda p: (p * 4 + zl * 2 + k) * B)
            self.y1 = Ring(net, buf, y, y_dev, lambda p: (p * 4 + other * 2 + k) * B)
            self.m_across = net.take(1)
            self.m_pair = net.take(8)

        def slot(self, rel, flip, core):
            return (lax.rem(y + rel, 4) * 4 + (other if flip else zl) * 2 + core) * B

        def share(self, rel, flip, src=None):
            ref = rows(self.buf, self.slot(rel, flip, k), B)
            net.send(ref if src is None else src, ref, self.m_pair + rel * 2 + flip, partner)

        def start(self):
            mine = rows(self.buf, self.slot(0, 0, k), B)
            net.send(self.own, mine, self.m_across, across)
            self.y0.start(self.own)
            self.share(0, 0, self.own)
            mine[...] = self.own[...]

        def crossed(self):
            net.recv(rows(self.buf, self.slot(0, 1, k), B), self.m_across)
            self.y1.start()
            self.share(0, 1)

        def near(self, flip):
            ring = self.y1 if flip else self.y0
            ring.from_left()
            self.share(3, flip)
            ring.from_right()
            self.share(1, flip)

        def far(self, flip):
            (self.y1 if flip else self.y0).from_far()
            self.share(2, flip)

        def paired(self):
            for rel in (0, 3, 1, 2):
                for flip in (0, 1):
                    net.recv(rows(self.buf, self.slot(rel, flip, 1 - k), B), self.m_pair + rel * 2 + flip)

    class Gather:
        def __init__(self, buf):
            self.z = Ring(net, buf, zh, z_dev, lambda p: (x * 4 + p) * B)
            self.x = {}
            for back in (0, 1, 3, 2):
                at = lax.rem(zh + 4 - back, 4)
                self.x[back] = Ring(net, buf, x, x_dev, lambda p, at=at: (p * 4 + at) * B)

    col_go, col_tok = Column(go, go_all), Column(tok, tok_all)
    row_hid, row_gg, row_gu = Gather(hid), Gather(gg), Gather(gu)
    grads = (row_gg, row_gu)
    own = row * B

    col_go.start()

    def make_hidden(i, _):
        at = pl.ds(pl.multiple_of(i * 16, 16), 16)
        g, u = gate[at, :].astype(F32), up[at, :].astype(F32)
        hid[pl.ds(pl.multiple_of(own + i * 16, 16), 16), :] = (g * jax.nn.sigmoid(g) * u).astype(BF)
        return 0

    lax.fori_loop(0, B // 16, make_hidden, 0)
    row_hid.x[0].start()
    row_hid.z.start()

    col_go.crossed()
    col_go.near(0)
    col_go.near(1)
    row_hid.x[0].neighbours()
    col_go.far(0)
    col_go.far(1)
    col_go.paired()
    col_tok.start()

    nn = ((1,), (0,))

    def share_of(group):
        return dot(go_all[pl.ds(pl.multiple_of(group * 512, 512), 512), :], dw[...], nn)

    s1[...] = share_of(xf).astype(BF)
    order = (2, 1, 3, 0)
    dest = [lax.rem(zh + off, 4) for off in order]
    m1l, m1r, m2l, m2r = (net.take(4) for _ in range(4))
    for i, zb in enumerate(dest):
        net.send(rows(s1, zb * B, H), rows(r1l, i * H, H), m1l + i, x_dev(xr))
        net.send(rows(s1, zb * B + H, H), rows(r1r, i * H, H), m1r + i, x_dev(xl))
    for group in (xr, xl, x):
        part[pl.ds(pl.multiple_of(group * 512, 512), 512), :] = share_of(group)

    col_tok.crossed()
    for i, zb in enumerate(dest):
        lo, hi = pl.ds(i * B, H), pl.ds(i * B + H, H)
        base = (xr * 4 + zb) * B
        s2r[hi, :] = part[pl.ds(pl.multiple_of(base + H, H), H), :].astype(BF)
        net.recv(rows(r1l, i * H, H), m1l + i)
        s2r[lo, :] = (part[pl.ds(pl.multiple_of(base, H), H), :] + r1l[pl.ds(i * H, H), :].astype(F32)).astype(BF)
        net.send(rows(s2r, i * B, B), rows(r2l, i * B, B), m2l + i, x_dev(xr))
        base = (xl * 4 + zb) * B
        s2l[lo, :] = part[pl.ds(pl.multiple_of(base, H), H), :].astype(BF)
        net.recv(rows(r1r, i * H, H), m1r + i)
        s2l[hi, :] = (part[pl.ds(pl.multiple_of(base + H, H), H), :] + r1r[pl.ds(i * H, H), :].astype(F32)).astype(BF)
        net.send(rows(s2l, i * B, B), rows(r2r, i * B, B), m2r + i, x_dev(xl))
    col_tok.near(0)
    col_tok.near(1)
    col_tok.far(0)
    col_tok.far(1)

    def x_sum(i):
        net.recv(rows(r2l, i * B, B), m2l + i)
        net.recv(rows(r2r, i * B, B), m2r + i)
        base = (x * 4 + dest[i]) * B
        at = pl.ds(i * B, B)
        return part[pl.ds(pl.multiple_of(base, B), B), :] + r2l[at, :].astype(F32) + r2r[at, :].astype(F32)

    mz = net.take(4)
    zs1[...] = x_sum(0).astype(BF)
    net.send(zs1.at[pl.ds(0, H), :], zr1l, mz, z_dev(zr))
    net.send(zs1.at[pl.ds(H, H), :], zr1r, mz + 1, z_dev(zlft))
    row_hid.z.neighbours()
    xs[...] = x_sum(1)
    net.recv(zr1l, mz)
    zs2r[pl.ds(0, H), :] = (xs[pl.ds(0, H), :] + zr1l[...].astype(F32)).astype(BF)
    zs2r[pl.ds(H, H), :] = xs[pl.ds(H, H), :].astype(BF)
    net.send(zs2r, zr2l, mz + 2, z_dev(zr))
    xs[...] = x_sum(2)
    net.recv(zr1r, mz + 1)
    zs2l[pl.ds(H, H), :] = (xs[pl.ds(H, H), :] + zr1r[...].astype(F32)).astype(BF)
    zs2l[pl.ds(0, H), :] = xs[pl.ds(0, H), :].astype(BF)
    net.send(zs2l, zr2r, mz + 3, z_dev(zlft))
    xs[...] = x_sum(3)
    row_hid.x[1].start()
    row_hid.x[0].from_far()
    net.recv(zr2l, mz + 2)
    net.recv(zr2r, mz + 3)

    def make_grads(i, _):
        at = pl.ds(pl.multiple_of(i * 16, 16), 16)
        to = pl.ds(pl.multiple_of(own + i * 16, 16), 16)
        g, u = gate[at, :].astype(F32), up[at, :].astype(F32)
        gh = xs[at, :] + zr2l[at, :].astype(F32) + zr2r[at, :].astype(F32)
        s = jax.nn.sigmoid(g)
        gu[to, :] = (gh * (g * s)).astype(BF)
        gg[to, :] = (gh * u * s * (1.0 + g * (1.0 - s))).astype(BF)
        return 0

    lax.fori_loop(0, B // 16, make_grads, 0)
    for a in grads:
        a.x[0].start()
        a.z.start()

    nt = ((1,), (1,))
    m_d2d, m_gt = net.take(8), net.take(8)
    late = []

    def block_rows(ref, j):
        return rows(ref, j * B, B)

    def token_block(group, back):
        return group * 4 + lax.rem(zh + 4 - back, 4)

    def gt_share(j):
        q = lax.div(j, 2)
        at = pl.ds(pl.multiple_of(j * B, B), B)
        here = pl.ds(pl.multiple_of(q * B, B), B)
        mine = lax.rem(j, 2) == k
        value = dot(gg[at, :], gw[...], nt) + dot(gu[at, :], uw[...], nt)

        @pl.when(mine)
        def _():
            gt_own[here, :] = value

        @pl.when(jnp.logical_not(mine))
        def _():
            d2d_s[here, :] = value
            net.copy(block_rows(d2d_s, q), block_rows(d2d_r, q), m_d2d + q, partner).start()

    def gt_finish(j):
        q = lax.div(j, 2)
        here = pl.ds(pl.multiple_of(q * B, B), B)
        to_y, to_z = lax.div(j, 4), lax.rem(q, 2)
        m = lax.rem(to_y - y + 4, 4) * 2 + lax.rem(to_z - zl + 2, 2)

        @pl.when(lax.rem(j, 2) == k)
        def _():
            net.recv(block_rows(d2d_r, q), m_d2d + q)
            value = gt_own[here, :] + d2d_r[here, :]

            @pl.when(m == 0)
            def _():
                gt_acc[...] = value

            @pl.when(m != 0)
            def _():
                gt_s[pl.ds(pl.multiple_of(m * B, B), B), :] = value.astype(BF)
                net.copy(block_rows(gt_s, m), block_rows(gt_r, m), m_gt + m, (row, to_y * 4 + to_z * 2 + k)).start()

    def gt(*blocks):
        for j in blocks:
            gt_share(j)
        for j in blocks:
            gt_finish(j)

    tn = ((0,), (0,))

    def weights(group, out, left, right, first=False):
        at = pl.ds(pl.multiple_of(group * 512, 512), 512)
        value = dot(left[at, :], right[at, :], tn)
        if first:
            out[...] = value
        else:
            out[...] += value

    gt(token_block(x, 0))
    for a in grads:
        a.x[0].neighbours()
    row_hid.x[1].neighbours()
    row_hid.x[3].start()
    gt(token_block(xl, 0), token_block(xr, 0))
    for a in grads:
        a.z.from_left()
        a.x[1].start()
        a.z.from_right()
        a.x[3].start()
    gt(token_block(x, 1), token_block(x, 3))
    col_tok.paired()
    for a in grads:
        a.x[0].from_far()
    gt(token_block(xf, 0))
    row_hid.z.from_far()
    for a in grads:
        a.x[1].neighbours()
    gt(token_block(xl, 1), token_block(xr, 1))
    for a in grads:
        a.x[3].neighbours()
    gt(token_block(xl, 3), token_block(xr, 3))
    for a in grads:
        a.z.from_far()
        a.x[2].start()
    gt(token_block(x, 2))
    weights(x, dgw, tok_all, gg, True)
    weights(x, duw, tok_all, gu, True)
    weights(x, ddw, go_all, hid, True)
    row_hid.x[3].neighbours()
    row_hid.x[1].from_far()
    for a in grads:
        a.x[1].from_far()
    gt(token_block(xf, 1))
    for a in grads:
        a.x[3].from_far()
    gt(token_block(xf, 3))
    for a in grads:
        a.x[2].neighbours()
    row_hid.x[2].start()
    gt(token_block(xl, 2), token_block(xr, 2))
    for group in (xl, xr):
        weights(group, dgw, tok_all, gg)
        weights(group, duw, tok_all, gu)
    for a in grads:
        a.x[2].from_far()
    gt(token_block(xf, 2))
    weights(xf, dgw, tok_all, gg)
    weights(xf, duw, tok_all, gu)
    row_hid.x[2].neighbours()
    row_hid.x[3].from_far()
    weights(xl, ddw, go_all, hid)
    weights(xr, ddw, go_all, hid)
    row_hid.x[2].from_far()
    weights(xf, ddw, go_all, hid)

    total = gt_acc[...]
    for m in range(1, 8):
        net.recv(block_rows(gt_r, m), m_gt + m)
        total = total + gt_r[pl.ds(m * B, B), :].astype(F32)
    gt_out[...] = total.astype(BF)

    net.drain()
    for q in range(8):
        net.copy(block_rows(d2d_s, q), block_rows(d2d_r, q), m_d2d + q, partner).wait_send()
    for m in range(1, 8):
        net.copy(block_rows(gt_s, m), block_rows(gt_r, m), m_gt + m, partner).wait_send()
    assert net.count <= N_MSG, net.count


def per_device(tokens, grad_out, gate, up, gate_weight, up_weight, down_weight):
    f, d = gate.shape[1], tokens.shape[1]
    vmem = pl.BlockSpec(memory_space=pltpu.VMEM)
    return pl.pallas_call(
        kernel,
        name="swiglu_backward",
        out_shape=(
            jax.ShapeDtypeStruct((B, d), BF),
            jax.ShapeDtypeStruct((d, f), F32),
            jax.ShapeDtypeStruct((d, f), F32),
            jax.ShapeDtypeStruct((d, f), F32),
        ),
        in_specs=[vmem] * 7,
        out_specs=(vmem,) * 4,
        scratch_shapes=[
            pltpu.VMEM((16 * B, d), BF), pltpu.VMEM((16 * B, d), BF),
            pltpu.VMEM((16 * B, f), BF), pltpu.VMEM((16 * B, f), BF), pltpu.VMEM((16 * B, f), BF),
            pltpu.VMEM((16 * B, f), F32),
            pltpu.VMEM((4 * B, f), BF), pltpu.VMEM((4 * B, f), BF), pltpu.VMEM((4 * B, f), BF),
            pltpu.VMEM((4 * H, f), BF), pltpu.VMEM((4 * H, f), BF),
            pltpu.VMEM((4 * B, f), BF), pltpu.VMEM((4 * B, f), BF),
            pltpu.VMEM((B, f), F32),
            pltpu.VMEM((B, f), BF), pltpu.VMEM((B, f), BF), pltpu.VMEM((B, f), BF),
            pltpu.VMEM((H, f), BF), pltpu.VMEM((H, f), BF),
            pltpu.VMEM((B, f), BF), pltpu.VMEM((B, f), BF),
            pltpu.VMEM((8 * B, d), F32), pltpu.VMEM((8 * B, d), F32), pltpu.VMEM((8 * B, d), F32),
            pltpu.VMEM((8 * B, d), BF), pltpu.VMEM((8 * B, d), BF),
            pltpu.VMEM((B, d), F32),
            pltpu.SemaphoreType.DMA((N_MSG,)), pltpu.SemaphoreType.DMA((N_MSG,)),
        ],
        compiler_params=pltpu.CompilerParams(
            collective_id=0, has_side_effects=True, vmem_limit_bytes=67_000_000
        ),
    )(tokens, grad_out, gate, up, gate_weight, up_weight, down_weight)


def solution(mesh):
    act, wide = P("col", "row"), P("row", "col")
    return jax.shard_map(
        per_device,
        mesh=mesh,
        in_specs=(act, act, wide, wide, wide, wide, wide),
        out_specs=(act, wide, wide, wide),
        check_vma=False,
    )
```

```python
import jax
import jax.numpy as jnp
from jax import lax
from jax.experimental import pallas as pl
from jax.experimental.pallas import tpu as pltpu
from jax.sharding import PartitionSpec as P

MESH = pl.DeviceIdType.MESH
BF = jnp.bfloat16
F32 = jnp.float32
B = 128
H = B // 2
N_MSG = 176
VMEM_LIMIT = 61_000_000
FIRST = 384


def rows(ref, start, size):
    return ref.at[pl.ds(pl.multiple_of(start, H), size), :]


class Net:
    def __init__(self, send, recv, me):
        self.send_sem, self.recv_sem, self.me = send, recv, me
        self.count = 0
        self.sent = []

    def take(self, n):
        first = self.count
        self.count += n
        return first

    def copy(self, src, dst, msg, device):
        return pltpu.make_async_remote_copy(
            src_ref=src, dst_ref=dst, send_sem=self.send_sem.at[msg], recv_sem=self.recv_sem.at[msg],
            device_id=device, device_id_type=MESH,
        )

    def send(self, src, dst, msg, device):
        copy = self.copy(src, dst, msg, device)
        copy.start()
        self.sent.append(copy)

    def recv(self, dst, msg):
        self.copy(dst, dst, msg, self.me).wait_recv()

    def drain(self):
        for copy in self.sent:
            copy.wait_send()


class Ring:
    def __init__(self, net, buf, pos, device_of, slot_of):
        self.net, self.buf, self.pos, self.device_of, self.slot_of = net, buf, pos, device_of, slot_of
        self.right, self.far, self.left = (lax.rem(pos + n, 4) for n in (1, 2, 3))
        self.msg = net.take(4)

    def start(self):
        own = rows(self.buf, self.slot_of(self.pos), B)
        self.net.send(own, own, self.msg, self.device_of(self.right))
        self.net.send(own, own, self.msg + 1, self.device_of(self.left))

    def from_left(self):
        slot = self.slot_of(self.left)
        self.net.recv(rows(self.buf, slot, B), self.msg)
        half = rows(self.buf, slot, H)
        self.net.send(half, half, self.msg + 2, self.device_of(self.right))

    def from_right(self):
        slot = self.slot_of(self.right)
        self.net.recv(rows(self.buf, slot, B), self.msg + 1)
        half = rows(self.buf, slot + H, H)
        self.net.send(half, half, self.msg + 3, self.device_of(self.left))

    def neighbours(self):
        self.from_left()
        self.from_right()

    def from_far(self):
        slot = self.slot_of(self.far)
        self.net.recv(rows(self.buf, slot, H), self.msg + 2)
        self.net.recv(rows(self.buf, slot + H, H), self.msg + 3)


def dot(a, b, dims):
    return lax.dot_general(a, b, (dims, ((), ())), preferred_element_type=F32)


def kernel(
    tok_in, go_in, gate_in, up_in, gw_in, uw_in, dw_in,
    gt_out, dgw, duw, ddw,
    gw, uw, dw, go_all, tok_all, gwt, uwt, gate_a, gate_b, up, gh, hid, gg, gu, part, s1, s2r, s2l, r1l, r1r, r2l, r2r,
    xs, zs1, zs2r, zs2l, zr1l, zr1r, zr2l, zr2r,
    gt_own, d2d_s, d2d_r, gt_s, gt_r, gt_acc,
    send_sem, recv_sem, load_sem,
):
    row, col = lax.axis_index("row"), lax.axis_index("col")
    x, zh = lax.div(row, 4), lax.rem(row, 4)
    y, zl, k = lax.div(col, 4), lax.rem(lax.div(col, 2), 2), lax.rem(col, 2)
    net = Net(send_sem, recv_sem, (row, col))
    other = 1 - zl

    def x_dev(p):
        return (p * 4 + zh, col)

    def z_dev(p):
        return (x * 4 + p, col)

    def y_dev(p):
        return (row, p * 4 + zl * 2 + k)

    partner = (row, y * 4 + zl * 2 + 1 - k)
    across = (row, y * 4 + other * 2 + k)
    xr, xf, xl = (lax.rem(x + n, 4) for n in (1, 2, 3))
    zr, zf, zlft = (lax.rem(zh + n, 4) for n in (1, 2, 3))

    barrier = pltpu.get_barrier_semaphore()
    peers = [x_dev(xr), x_dev(xl), z_dev(zr), z_dev(zlft), partner, across]
    for dy in (1, 2, 3):
        p = lax.rem(y + dy, 4)
        peers += [(row, p * 4 + zl * 2 + k), (row, p * 4 + other * 2 + k)]
    for peer in peers:
        pl.semaphore_signal(barrier, inc=1, device_id=peer, device_id_type=MESH)

    own = row * B
    sources = [
        (go_in, rows(go_all, col * B, B)),
        (up_in, rows(up, own, B)),
        (gate_in.at[:, pl.ds(FIRST, gate_in.shape[1] - FIRST)], rows(gate_b, own, B)),
        (gate_in.at[:, pl.ds(0, FIRST)], rows(gate_a, own, B)),
        (dw_in, dw),
        (tok_in, rows(tok_all, col * B, B)),
        (gw_in, gw),
        (uw_in, uw),
    ]
    loads = [pltpu.make_async_copy(src, dst, load_sem.at[i]) for i, (src, dst) in enumerate(sources)]
    for load in loads:
        load.start()
    pl.semaphore_wait(barrier, len(peers))

    class Column:
        def __init__(self, buf):
            self.buf = buf
            self.y0 = Ring(net, buf, y, y_dev, lambda p: (p * 4 + zl * 2 + k) * B)
            self.y1 = Ring(net, buf, y, y_dev, lambda p: (p * 4 + other * 2 + k) * B)
            self.m_across = net.take(1)
            self.m_pair = net.take(8)

        def slot(self, rel, flip, core):
            return (lax.rem(y + rel, 4) * 4 + (other if flip else zl) * 2 + core) * B

        def share(self, rel, flip):
            ref = rows(self.buf, self.slot(rel, flip, k), B)
            net.send(ref, ref, self.m_pair + rel * 2 + flip, partner)

        def start(self):
            mine = rows(self.buf, self.slot(0, 0, k), B)
            net.send(mine, mine, self.m_across, across)
            self.y0.start()
            self.share(0, 0)

        def crossed(self):
            net.recv(rows(self.buf, self.slot(0, 1, k), B), self.m_across)
            self.y1.start()
            self.share(0, 1)

        def near(self, flip):
            ring = self.y1 if flip else self.y0
            ring.from_left()
            self.share(3, flip)
            ring.from_right()
            self.share(1, flip)

        def far(self, flip):
            (self.y1 if flip else self.y0).from_far()
            self.share(2, flip)

        def paired(self):
            for rel in (0, 3, 1, 2):
                for flip in (0, 1):
                    net.recv(rows(self.buf, self.slot(rel, flip, 1 - k), B), self.m_pair + rel * 2 + flip)

    class Gather:
        def __init__(self, buf):
            self.z = Ring(net, buf, zh, z_dev, lambda p: (x * 4 + p) * B)
            self.x = {}
            for back in (0, 1, 3, 2):
                at = lax.rem(zh + 4 - back, 4)
                self.x[back] = Ring(net, buf, x, x_dev, lambda p, at=at: (p * 4 + at) * B)

    col_go, col_tok = Column(go_all), Column(tok_all)
    row_up, row_gb, row_gh = Gather(up), Gather(gate_b), Gather(gh)
    ga_x = Ring(net, gate_a, x, x_dev, lambda p: (p * 4 + zh) * B)
    ga_z, ga_zl, ga_zr, ga_zf = (
        Ring(net, gate_a, zh, z_dev, lambda p, group=group: (group * 4 + p) * B) for group in (x, xl, xr, xf)
    )

    loads[0].wait()
    col_go.start()
    loads[1].wait()
    row_up.x[0].start()
    loads[2].wait()
    row_gb.x[0].start()
    loads[3].wait()
    ga_x.start()
    col_go.crossed()
    row_up.z.start()
    row_gb.z.start()
    col_go.near(0)
    row_up.x[0].neighbours()
    col_go.near(1)
    row_gb.x[0].neighbours()
    col_go.far(0)
    ga_x.neighbours()
    col_go.far(1)
    loads[4].wait()
    col_go.paired()

    nn = ((1,), (0,))

    def share_of(group):
        return dot(go_all[pl.ds(pl.multiple_of(group * 512, 512), 512), :], dw[...], nn)

    s1[...] = share_of(xf).astype(BF)
    order = (2, 1, 3, 0)
    dest = [lax.rem(zh + off, 4) for off in order]
    m1l, m1r, m2l, m2r = (net.take(4) for _ in range(4))
    for i, zb in enumerate(dest):
        net.send(rows(s1, zb * B, H), rows(r1l, i * H, H), m1l + i, x_dev(xr))
        net.send(rows(s1, zb * B + H, H), rows(r1r, i * H, H), m1r + i, x_dev(xl))
    for group in (xr, xl, x):
        part[pl.ds(pl.multiple_of(group * 512, 512), 512), :] = share_of(group)

    loads[5].wait()
    col_tok.start()
    row_up.z.neighbours()
    ga_z.start()
    for i, zb in enumerate(dest):
        lo, hi = pl.ds(i * B, H), pl.ds(i * B + H, H)
        base = (xr * 4 + zb) * B
        s2r[hi, :] = part[pl.ds(pl.multiple_of(base + H, H), H), :].astype(BF)
        net.recv(rows(r1l, i * H, H), m1l + i)
        s2r[lo, :] = (part[pl.ds(pl.multiple_of(base, H), H), :] + r1l[pl.ds(i * H, H), :].astype(F32)).astype(BF)
        net.send(rows(s2r, i * B, B), rows(r2l, i * B, B), m2l + i, x_dev(xr))
        base = (xl * 4 + zb) * B
        s2l[lo, :] = part[pl.ds(pl.multiple_of(base, H), H), :].astype(BF)
        net.recv(rows(r1r, i * H, H), m1r + i)
        s2l[hi, :] = (part[pl.ds(pl.multiple_of(base + H, H), H), :] + r1r[pl.ds(i * H, H), :].astype(F32)).astype(BF)
        net.send(rows(s2l, i * B, B), rows(r2r, i * B, B), m2r + i, x_dev(xl))
        if i == 1:
            row_gb.z.neighbours()
    col_tok.crossed()
    row_up.x[1].start()

    def x_sum(i):
        net.recv(rows(r2l, i * B, B), m2l + i)
        net.recv(rows(r2r, i * B, B), m2r + i)
        base = (x * 4 + dest[i]) * B
        at = pl.ds(i * B, B)
        return part[pl.ds(pl.multiple_of(base, B), B), :] + r2l[at, :].astype(F32) + r2r[at, :].astype(F32)

    mz = net.take(6)
    lo, hi = pl.ds(0, H), pl.ds(H, H)
    zs1[...] = x_sum(0).astype(BF)
    net.send(zs1.at[lo, :], zr1l, mz, z_dev(zr))
    net.send(zs1.at[hi, :], zr1r, mz + 1, z_dev(zlft))
    col_tok.near(0)
    row_up.x[3].start()
    loads[6].wait()
    loads[7].wait()
    gwt[...] = gw[...].T
    uwt[...] = uw[...].T
    xs[...] = x_sum(1)
    zs2r[hi, :] = xs[hi, :].astype(BF)
    net.send(zs2r.at[hi, :], zr2l.at[hi, :], mz + 2, z_dev(zr))
    net.recv(zr1l, mz)
    zs2r[lo, :] = (xs[lo, :] + zr1l[...].astype(F32)).astype(BF)
    net.send(zs2r.at[lo, :], zr2l.at[lo, :], mz + 3, z_dev(zr))
    xs[...] = x_sum(2)
    zs2l[lo, :] = xs[lo, :].astype(BF)
    net.send(zs2l.at[lo, :], zr2r.at[lo, :], mz + 4, z_dev(zlft))
    net.recv(zr1r, mz + 1)
    zs2l[hi, :] = (xs[hi, :] + zr1r[...].astype(F32)).astype(BF)
    net.send(zs2l.at[hi, :], zr2r.at[hi, :], mz + 5, z_dev(zlft))
    row_gb.x[1].start()
    row_gb.x[3].start()
    xs[...] = x_sum(3)
    net.recv(zr2l.at[hi, :], mz + 2)
    net.recv(zr2l.at[lo, :], mz + 3)
    net.recv(zr2r.at[lo, :], mz + 4)
    net.recv(zr2r.at[hi, :], mz + 5)

    gh[pl.ds(pl.multiple_of(own, B), B), :] = (xs[...] + zr2l[...].astype(F32) + zr2r[...].astype(F32)).astype(BF)
    row_gh.x[0].start()
    row_gh.z.start()
    ga_z.neighbours()
    col_tok.near(1)

    width = hid.shape[1]
    parts = ((gate_a, pl.ds(0, FIRST)), (gate_b, pl.ds(FIRST, width - FIRST)))

    def elementwise(j):
        def some(i, _):
            at = pl.ds(pl.multiple_of(j * B + i * 16, 16), 16)
            for gate, cols in parts:
                g, u, d = gate[at, :].astype(F32), up[at, cols].astype(F32), gh[at, cols].astype(F32)
                s = jax.nn.sigmoid(g)
                active = g * s
                hid[at, cols] = (active * u).astype(BF)
                gu[at, cols] = (d * active).astype(BF)
                gg[at, cols] = (d * u * s * (1.0 + g * (1.0 - s))).astype(BF)
            return 0

        lax.fori_loop(0, B // 16, some, 0)

    m_d2d, m_gt = net.take(8), net.take(8)

    def block_rows(ref, j):
        return rows(ref, j * B, B)

    def token_block(group, back):
        return group * 4 + lax.rem(zh + 4 - back, 4)

    def gt_share(j):
        q = lax.div(j, 2)
        at = pl.ds(pl.multiple_of(j * B, B), B)
        here = pl.ds(pl.multiple_of(q * B, B), B)
        mine = lax.rem(j, 2) == k
        elementwise(j)
        value = dot(gg[at, :], gwt[...], nn) + dot(gu[at, :], uwt[...], nn)

        @pl.when(mine)
        def _():
            gt_own[here, :] = value

        @pl.when(jnp.logical_not(mine))
        def _():
            d2d_s[here, :] = value
            net.copy(block_rows(d2d_s, q), block_rows(d2d_r, q), m_d2d + q, partner).start()

    def gt_finish(j):
        q = lax.div(j, 2)
        here = pl.ds(pl.multiple_of(q * B, B), B)
        to_y, to_z = lax.div(j, 4), lax.rem(q, 2)
        m = lax.rem(to_y - y + 4, 4) * 2 + lax.rem(to_z - zl + 2, 2)

        @pl.when(lax.rem(j, 2) == k)
        def _():
            net.recv(block_rows(d2d_r, q), m_d2d + q)
            value = gt_own[here, :] + d2d_r[here, :]

            @pl.when(m == 0)
            def _():
                gt_acc[...] = value

            @pl.when(m != 0)
            def _():
                gt_s[pl.ds(pl.multiple_of(m * B, B), B), :] = value.astype(BF)
                net.copy(block_rows(gt_s, m), block_rows(gt_r, m), m_gt + m, (row, to_y * 4 + to_z * 2 + k)).start()

    def gt(*blocks):
        for j in blocks:
            gt_share(j)
        for j in blocks:
            gt_finish(j)

    tn = ((0,), (0,))

    def weights(group, out, left, right, first=False):
        at = pl.ds(pl.multiple_of(group * 512, 512), 512)
        value = dot(left[at, :], right[at, :], tn)
        if first:
            out[...] = value
        else:
            out[...] += value

    def all_weights(group, first=False):
        weights(group, dgw, tok_all, gg, first)
        weights(group, duw, tok_all, gu, first)
        weights(group, ddw, go_all, hid, first)

    gt(token_block(x, 0))
    row_up.x[1].neighbours()
    row_up.x[3].neighbours()
    row_up.z.from_far()
    row_gb.z.from_far()
    row_up.x[2].start()
    row_gh.z.from_left()
    row_gh.x[1].start()
    row_gh.z.from_right()
    row_gh.x[3].start()
    ga_zl.start()
    row_gb.x[1].neighbours()
    row_gb.x[3].neighbours()
    row_gh.x[0].neighbours()
    row_gb.x[2].start()
    gt(token_block(x, 1), token_block(x, 3))
    row_gh.z.from_far()
    row_gh.x[2].start()
    ga_zr.start()
    gt(token_block(xl, 0), token_block(xr, 0))
    ga_zl.neighbours()
    ga_x.from_far()
    ga_zf.start()
    row_up.x[2].neighbours()
    col_tok.far(0)
    col_tok.far(1)
    row_up.x[0].from_far()
    row_gb.x[0].from_far()
    row_gh.x[0].from_far()
    gt(token_block(xf, 0))
    ga_z.from_far()
    gt(token_block(x, 2))
    col_tok.paired()
    ga_zr.neighbours()
    row_gh.x[1].neighbours()
    gt(token_block(xl, 1), token_block(xr, 1))
    row_gb.x[2].neighbours()
    all_weights(x, True)
    row_gh.x[3].neighbours()
    gt(token_block(xl, 3), token_block(xr, 3))
    ga_zf.neighbours()
    for a in (row_up, row_gb):
        a.x[1].from_far()
        a.x[3].from_far()
    row_gh.x[2].neighbours()
    ga_zl.from_far()
    ga_zr.from_far()
    gt(token_block(xl, 2), token_block(xr, 2))
    row_gh.x[1].from_far()
    gt(token_block(xf, 1))
    all_weights(xl)
    row_gh.x[3].from_far()
    gt(token_block(xf, 3))
    all_weights(xr)
    for a in (row_up, row_gb):
        a.x[2].from_far()
    ga_zf.from_far()
    row_gh.x[2].from_far()
    last = token_block(xf, 2)
    gt_share(last)
    weights(xf, dgw, tok_all, gg)
    gt_finish(last)
    weights(xf, duw, tok_all, gu)
    weights(xf, ddw, go_all, hid)

    total = gt_acc[...]
    for m in range(1, 8):
        net.recv(block_rows(gt_r, m), m_gt + m)
        total = total + gt_r[pl.ds(m * B, B), :].astype(F32)
    gt_out[...] = total.astype(BF)

    net.drain()
    for q in range(8):
        net.copy(block_rows(d2d_s, q), block_rows(d2d_r, q), m_d2d + q, partner).wait_send()
    for m in range(1, 8):
        net.copy(block_rows(gt_s, m), block_rows(gt_r, m), m_gt + m, partner).wait_send()
    assert net.count <= N_MSG, net.count


def hand_over(*results):
    def body(*refs):
        copies = [pltpu.make_async_copy(src, dst, refs[8].at[i]) for i, (src, dst) in enumerate(zip(refs[:4], refs[4:8]))]
        for copy in copies:
            copy.start()
        for copy in copies:
            copy.wait()

    hbm = pl.BlockSpec(memory_space=pltpu.HBM)
    vmem = pl.BlockSpec(memory_space=pltpu.VMEM)
    return pl.pallas_call(
        body,
        name="hand_over",
        in_specs=[vmem] * 4,
        out_specs=(hbm,) * 4,
        out_shape=tuple(jax.ShapeDtypeStruct(a.shape, a.dtype) for a in results),
        scratch_shapes=[pltpu.SemaphoreType.DMA((4,))],
        compiler_params=pltpu.CompilerParams(vmem_limit_bytes=16 * 1024 * 1024),
    )(*results)


def per_device(tokens, grad_out, gate, up, gate_weight, up_weight, down_weight):
    f, d = gate.shape[1], tokens.shape[1]
    vmem = pl.BlockSpec(memory_space=pltpu.VMEM)
    hbm = pl.BlockSpec(memory_space=pltpu.HBM)
    results = pl.pallas_call(
        kernel,
        name="swiglu_backward",
        out_shape=(
            pltpu.VMEM((B, d), BF),
            pltpu.VMEM((d, f), F32),
            pltpu.VMEM((d, f), F32),
            pltpu.VMEM((d, f), F32),
        ),
        in_specs=[hbm] * 7,
        out_specs=(vmem,) * 4,
        scratch_shapes=[
            pltpu.VMEM((d, f), BF), pltpu.VMEM((d, f), BF), pltpu.VMEM((d, f), BF),
            pltpu.VMEM((16 * B, d), BF), pltpu.VMEM((16 * B, d), BF),
            pltpu.VMEM((f, d), BF), pltpu.VMEM((f, d), BF),
            pltpu.VMEM((16 * B, FIRST), BF), pltpu.VMEM((16 * B, f - FIRST), BF),
            pltpu.VMEM((16 * B, f), BF), pltpu.VMEM((16 * B, f), BF),
            pltpu.VMEM((16 * B, f), BF), pltpu.VMEM((16 * B, f), BF), pltpu.VMEM((16 * B, f), BF),
            pltpu.VMEM((16 * B, f), F32),
            pltpu.VMEM((4 * B, f), BF), pltpu.VMEM((4 * B, f), BF), pltpu.VMEM((4 * B, f), BF),
            pltpu.VMEM((4 * H, f), BF), pltpu.VMEM((4 * H, f), BF),
            pltpu.VMEM((4 * B, f), BF), pltpu.VMEM((4 * B, f), BF),
            pltpu.VMEM((B, f), F32),
            pltpu.VMEM((B, f), BF), pltpu.VMEM((B, f), BF), pltpu.VMEM((B, f), BF),
            pltpu.VMEM((H, f), BF), pltpu.VMEM((H, f), BF),
            pltpu.VMEM((B, f), BF), pltpu.VMEM((B, f), BF),
            pltpu.VMEM((8 * B, d), F32), pltpu.VMEM((8 * B, d), F32), pltpu.VMEM((8 * B, d), F32),
            pltpu.VMEM((8 * B, d), BF), pltpu.VMEM((8 * B, d), BF),
            pltpu.VMEM((B, d), F32),
            pltpu.SemaphoreType.DMA((N_MSG,)), pltpu.SemaphoreType.DMA((N_MSG,)), pltpu.SemaphoreType.DMA((8,)),
        ],
        compiler_params=pltpu.CompilerParams(
            collective_id=0, has_side_effects=True, vmem_limit_bytes=VMEM_LIMIT
        ),
    )(tokens, grad_out, gate, up, gate_weight, up_weight, down_weight)
    return hand_over(*results)


def solution(mesh):
    act, wide = P("col", "row"), P("row", "col")
    return jax.shard_map(
        per_device,
        mesh=mesh,
        in_specs=(act, act, wide, wide, wide, wide, wide),
        out_specs=(act, wide, wide, wide),
        check_vma=False,
    )
```

```python
import jax
import jax.numpy as jnp
from jax import lax
from jax.experimental import pallas as pl
from jax.experimental.pallas import tpu as pltpu
from jax.sharding import PartitionSpec as P

MESH = pl.DeviceIdType.MESH
BF = jnp.bfloat16
F32 = jnp.float32
B = 128
H = B // 2
N_MSG = 176
VMEM_LIMIT = 61_000_000
FIRST = 512


def rows(ref, start, size):
    return ref.at[pl.ds(pl.multiple_of(start, H), size), :]


class Net:
    def __init__(self, send, recv, me):
        self.send_sem, self.recv_sem, self.me = send, recv, me
        self.count = 0
        self.sent = []

    def take(self, n):
        first = self.count
        self.count += n
        return first

    def copy(self, src, dst, msg, device):
        return pltpu.make_async_remote_copy(
            src_ref=src, dst_ref=dst, send_sem=self.send_sem.at[msg], recv_sem=self.recv_sem.at[msg],
            device_id=device, device_id_type=MESH,
        )

    def send(self, src, dst, msg, device):
        copy = self.copy(src, dst, msg, device)
        copy.start()
        self.sent.append(copy)

    def recv(self, dst, msg):
        self.copy(dst, dst, msg, self.me).wait_recv()

    def drain(self):
        for copy in self.sent:
            copy.wait_send()


class Ring:
    def __init__(self, net, buf, pos, device_of, slot_of, split=False):
        self.net, self.buf, self.pos, self.device_of, self.slot_of = net, buf, pos, device_of, slot_of
        self.right, self.far, self.left = (lax.rem(pos + n, 4) for n in (1, 2, 3))
        self.split = split
        self.msg = net.take(6 if split else 4)

    def start(self):
        slot = self.slot_of(self.pos)
        first, second, own = rows(self.buf, slot, H), rows(self.buf, slot + H, H), rows(self.buf, slot, B)
        right, left = self.device_of(self.right), self.device_of(self.left)
        self.net.send(first if self.split else own, first if self.split else own, self.msg, right)
        self.net.send(second if self.split else own, second if self.split else own, self.msg + 1, left)
        if self.split:
            self.net.send(second, second, self.msg + 4, right)
            self.net.send(first, first, self.msg + 5, left)

    def from_left(self):
        slot = self.slot_of(self.left)
        half = rows(self.buf, slot, H)
        self.net.recv(half if self.split else rows(self.buf, slot, B), self.msg)
        self.net.send(half, half, self.msg + 2, self.device_of(self.right))

    def from_right(self):
        slot = self.slot_of(self.right)
        half = rows(self.buf, slot + H, H)
        self.net.recv(half if self.split else rows(self.buf, slot, B), self.msg + 1)
        self.net.send(half, half, self.msg + 3, self.device_of(self.left))

    def neighbours(self):
        self.from_left()
        self.from_right()

    def rest(self):
        self.net.recv(rows(self.buf, self.slot_of(self.left) + H, H), self.msg + 4)
        self.net.recv(rows(self.buf, self.slot_of(self.right), H), self.msg + 5)

    def from_far(self):
        slot = self.slot_of(self.far)
        self.net.recv(rows(self.buf, slot, H), self.msg + 2)
        self.net.recv(rows(self.buf, slot + H, H), self.msg + 3)


def dot(a, b, dims):
    return lax.dot_general(a, b, (dims, ((), ())), preferred_element_type=F32)


def kernel(
    tok_in, go_in, gate_in, up_in, gw_in, uw_in, dw_in,
    gt_out, dgw, duw, ddw,
    gw, uw, dw, go_all, tok_all, gwt, uwt, gate_a, gate_b, up, gh, hid, gg, gu, part, s1, s2r, s2l, r1l, r1r, r2l, r2r,
    xs, zs1, zs2r, zs2l, zr1l, zr1r, zr2l, zr2r,
    gt_own, d2d_s, d2d_r, gt_s, gt_r, gt_acc,
    send_sem, recv_sem, load_sem,
):
    row, col = lax.axis_index("row"), lax.axis_index("col")
    y, zl, k = lax.div(col, 4), lax.rem(lax.div(col, 2), 2), lax.rem(col, 2)

    def turned(p):
        return p + zl * (3 - 2 * p)

    x, zh = lax.div(row, 4), turned(lax.rem(row, 4))
    net = Net(send_sem, recv_sem, (row, col))
    other = 1 - zl

    def x_dev(p):
        return (p * 4 + turned(zh), col)

    def z_dev(p):
        return (x * 4 + turned(p), col)

    def y_dev(p):
        return (row, p * 4 + zl * 2 + k)

    partner = (row, y * 4 + zl * 2 + 1 - k)
    across = (row, y * 4 + other * 2 + k)
    xr, xf, xl = (lax.rem(x + n, 4) for n in (1, 2, 3))
    zr, zf, zlft = (lax.rem(zh + n, 4) for n in (1, 2, 3))

    barrier = pltpu.get_barrier_semaphore()
    peers = [x_dev(xr), x_dev(xl), z_dev(zr), z_dev(zlft), partner, across]
    for dy in (1, 2, 3):
        p = lax.rem(y + dy, 4)
        peers += [(row, p * 4 + zl * 2 + k), (row, p * 4 + other * 2 + k)]
    for peer in peers:
        pl.semaphore_signal(barrier, inc=1, device_id=peer, device_id_type=MESH)

    own = row * B
    sources = [
        (go_in, rows(go_all, col * B, B)),
        (up_in, rows(up, own, B)),
        (gate_in.at[:, pl.ds(FIRST, gate_in.shape[1] - FIRST)], rows(gate_b, own, B)),
        (gate_in.at[:, pl.ds(0, FIRST)], rows(gate_a, own, B)),
        (dw_in, dw),
        (tok_in, rows(tok_all, col * B, B)),
        (gw_in, gw),
        (uw_in, uw),
    ]
    loads = [pltpu.make_async_copy(src, dst, load_sem.at[i]) for i, (src, dst) in enumerate(sources)]
    for load in loads:
        load.start()
    pl.semaphore_wait(barrier, len(peers))

    class Column:
        def __init__(self, buf):
            self.buf = buf
            self.y0 = Ring(net, buf, y, y_dev, lambda p: (p * 4 + zl * 2 + k) * B)
            self.y1 = Ring(net, buf, y, y_dev, lambda p: (p * 4 + other * 2 + k) * B)
            self.m_across = net.take(1)
            self.m_pair = net.take(8)

        def slot(self, rel, flip, core):
            return (lax.rem(y + rel, 4) * 4 + (other if flip else zl) * 2 + core) * B

        def share(self, rel, flip):
            ref = rows(self.buf, self.slot(rel, flip, k), B)
            net.send(ref, ref, self.m_pair + rel * 2 + flip, partner)

        def start(self):
            mine = rows(self.buf, self.slot(0, 0, k), B)
            net.send(mine, mine, self.m_across, across)
            self.y0.start()
            self.share(0, 0)

        def crossed(self):
            net.recv(rows(self.buf, self.slot(0, 1, k), B), self.m_across)
            self.y1.start()
            self.share(0, 1)

        def near(self, flip):
            ring = self.y1 if flip else self.y0
            ring.from_left()
            self.share(3, flip)
            ring.from_right()
            self.share(1, flip)

        def far(self, flip):
            (self.y1 if flip else self.y0).from_far()
            self.share(2, flip)

        def paired(self):
            for rel in (0, 3, 1, 2):
                for flip in (0, 1):
                    net.recv(rows(self.buf, self.slot(rel, flip, 1 - k), B), self.m_pair + rel * 2 + flip)

    class Gather:
        def __init__(self, buf, split=()):
            self.z = Ring(net, buf, zh, z_dev, lambda p: (x * 4 + turned(p)) * B)
            self.x = {}
            for back in (0, 1, 3, 2):
                at = turned(lax.rem(zh + 4 - back, 4))
                self.x[back] = Ring(net, buf, x, x_dev, lambda p, at=at: (p * 4 + at) * B, back in split)

    col_go, col_tok = Column(go_all), Column(tok_all)
    row_up, row_gb, row_gh = Gather(up), Gather(gate_b), Gather(gh, (2,))
    ga_x = Ring(net, gate_a, x, x_dev, lambda p: (p * 4 + turned(zh)) * B)
    ga_z, ga_zl, ga_zr, ga_zf = (
        Ring(net, gate_a, zh, z_dev, lambda p, group=group: (group * 4 + turned(p)) * B) for group in (x, xl, xr, xf)
    )

    loads[0].wait()
    col_go.start()
    loads[1].wait()
    row_up.x[0].start()
    loads[2].wait()
    row_gb.x[0].start()
    loads[3].wait()
    ga_x.start()
    col_go.crossed()
    row_up.z.start()
    row_gb.z.start()
    col_go.near(0)
    row_up.x[0].neighbours()
    col_go.near(1)
    row_gb.x[0].neighbours()
    col_go.far(0)
    ga_x.neighbours()
    col_go.far(1)
    loads[4].wait()
    col_go.paired()

    nn = ((1,), (0,))

    def share_of(group):
        return dot(go_all[pl.ds(pl.multiple_of(group * 512, 512), 512), :], dw[...], nn)

    s1[...] = share_of(xf).astype(BF)
    order = (2, 1, 3, 0)
    dest = [turned(lax.rem(zh + off, 4)) for off in order]
    m1l, m1r, m2l, m2r = (net.take(4) for _ in range(4))
    for i, zb in enumerate(dest):
        net.send(rows(s1, zb * B, H), rows(r1l, i * H, H), m1l + i, x_dev(xr))
        net.send(rows(s1, zb * B + H, H), rows(r1r, i * H, H), m1r + i, x_dev(xl))
    for group in (xr, xl, x):
        part[pl.ds(pl.multiple_of(group * 512, 512), 512), :] = share_of(group)

    loads[5].wait()
    col_tok.start()
    row_up.z.neighbours()
    ga_z.start()
    for i, zb in enumerate(dest):
        lo, hi = pl.ds(i * B, H), pl.ds(i * B + H, H)
        base = (xr * 4 + zb) * B
        s2r[hi, :] = part[pl.ds(pl.multiple_of(base + H, H), H), :].astype(BF)
        net.recv(rows(r1l, i * H, H), m1l + i)
        s2r[lo, :] = (part[pl.ds(pl.multiple_of(base, H), H), :] + r1l[pl.ds(i * H, H), :].astype(F32)).astype(BF)
        net.send(rows(s2r, i * B, B), rows(r2l, i * B, B), m2l + i, x_dev(xr))
        base = (xl * 4 + zb) * B
        s2l[lo, :] = part[pl.ds(pl.multiple_of(base, H), H), :].astype(BF)
        net.recv(rows(r1r, i * H, H), m1r + i)
        s2l[hi, :] = (part[pl.ds(pl.multiple_of(base + H, H), H), :] + r1r[pl.ds(i * H, H), :].astype(F32)).astype(BF)
        net.send(rows(s2l, i * B, B), rows(r2r, i * B, B), m2r + i, x_dev(xl))
        if i == 1:
            row_gb.z.neighbours()
    col_tok.crossed()
    row_up.x[1].start()

    def x_sum(i):
        net.recv(rows(r2l, i * B, B), m2l + i)
        net.recv(rows(r2r, i * B, B), m2r + i)
        base = (x * 4 + dest[i]) * B
        at = pl.ds(i * B, B)
        return part[pl.ds(pl.multiple_of(base, B), B), :] + r2l[at, :].astype(F32) + r2r[at, :].astype(F32)

    mz = net.take(6)
    lo, hi = pl.ds(0, H), pl.ds(H, H)
    zs1[...] = x_sum(0).astype(BF)
    net.send(zs1.at[lo, :], zr1l, mz, z_dev(zr))
    net.send(zs1.at[hi, :], zr1r, mz + 1, z_dev(zlft))
    col_tok.near(0)
    row_up.x[3].start()
    loads[6].wait()
    loads[7].wait()
    gwt[...] = gw[...].T
    uwt[...] = uw[...].T
    xs[...] = x_sum(1)
    zs2r[hi, :] = xs[hi, :].astype(BF)
    net.send(zs2r.at[hi, :], zr2l.at[hi, :], mz + 2, z_dev(zr))
    net.recv(zr1l, mz)
    zs2r[lo, :] = (xs[lo, :] + zr1l[...].astype(F32)).astype(BF)
    net.send(zs2r.at[lo, :], zr2l.at[lo, :], mz + 3, z_dev(zr))
    xs[...] = x_sum(2)
    zs2l[lo, :] = xs[lo, :].astype(BF)
    net.send(zs2l.at[lo, :], zr2r.at[lo, :], mz + 4, z_dev(zlft))
    net.recv(zr1r, mz + 1)
    zs2l[hi, :] = (xs[hi, :] + zr1r[...].astype(F32)).astype(BF)
    net.send(zs2l.at[hi, :], zr2r.at[hi, :], mz + 5, z_dev(zlft))
    row_gb.x[1].start()
    row_gb.x[3].start()
    xs[...] = x_sum(3)
    net.recv(zr2l.at[hi, :], mz + 2)
    net.recv(zr2l.at[lo, :], mz + 3)
    net.recv(zr2r.at[lo, :], mz + 4)
    net.recv(zr2r.at[hi, :], mz + 5)

    gh[pl.ds(pl.multiple_of(own, B), B), :] = (xs[...] + zr2l[...].astype(F32) + zr2r[...].astype(F32)).astype(BF)
    row_gh.x[0].start()
    row_gh.z.start()
    ga_z.neighbours()
    col_tok.near(1)

    width = hid.shape[1]
    parts = ((gate_a, pl.ds(0, FIRST)), (gate_b, pl.ds(FIRST, width - FIRST)))

    def elementwise(j):
        def some(i, _):
            at = pl.ds(pl.multiple_of(j * B + i * 16, 16), 16)
            for gate, cols in parts:
                g, u, d = gate[at, :].astype(F32), up[at, cols].astype(F32), gh[at, cols].astype(F32)
                s = jax.nn.sigmoid(g)
                active = g * s
                hid[at, cols] = (active * u).astype(BF)
                gu[at, cols] = (d * active).astype(BF)
                gg[at, cols] = (d * u * s * (1.0 + g * (1.0 - s))).astype(BF)
            return 0

        lax.fori_loop(0, B // 16, some, 0)

    m_d2d, m_gt = net.take(8), net.take(8)

    def block_rows(ref, j):
        return rows(ref, j * B, B)

    def token_block(group, back):
        return group * 4 + turned(lax.rem(zh + 4 - back, 4))

    def gt_share(j):
        q = lax.div(j, 2)
        at = pl.ds(pl.multiple_of(j * B, B), B)
        here = pl.ds(pl.multiple_of(q * B, B), B)
        mine = lax.rem(j, 2) == k
        elementwise(j)
        value = dot(gg[at, :], gwt[...], nn) + dot(gu[at, :], uwt[...], nn)

        @pl.when(mine)
        def _():
            gt_own[here, :] = value

        @pl.when(jnp.logical_not(mine))
        def _():
            d2d_s[here, :] = value
            net.copy(block_rows(d2d_s, q), block_rows(d2d_r, q), m_d2d + q, partner).start()

    def gt_finish(j):
        q = lax.div(j, 2)
        here = pl.ds(pl.multiple_of(q * B, B), B)
        to_y, to_z = lax.div(j, 4), lax.rem(q, 2)
        m = lax.rem(to_y - y + 4, 4) * 2 + lax.rem(to_z - zl + 2, 2)

        @pl.when(lax.rem(j, 2) == k)
        def _():
            net.recv(block_rows(d2d_r, q), m_d2d + q)
            value = gt_own[here, :] + d2d_r[here, :]

            @pl.when(m == 0)
            def _():
                gt_acc[...] = value

            @pl.when(m != 0)
            def _():
                gt_s[pl.ds(pl.multiple_of(m * B, B), B), :] = value.astype(BF)
                net.copy(block_rows(gt_s, m), block_rows(gt_r, m), m_gt + m, (row, to_y * 4 + to_z * 2 + k)).start()

    def gt(*blocks):
        for j in blocks:
            gt_share(j)
        for j in blocks:
            gt_finish(j)

    tn = ((0,), (0,))

    early = lax.div(turned(zh), 2)
    late = 1 - early

    def weights(group, pair, first=False):
        at = pl.ds(pl.multiple_of(group * 512 + pair * 256, 256), 256)
        for out, left, right in ((dgw, tok_all, gg), (duw, tok_all, gu), (ddw, go_all, hid)):
            value = dot(left[at, :], right[at, :], tn)
            if first:
                out[...] = value
            else:
                out[...] += value

    gt(token_block(x, 0))
    row_up.x[1].neighbours()
    row_up.x[3].neighbours()
    row_up.z.from_far()
    row_gb.z.from_far()
    row_up.x[2].start()
    row_gh.z.from_left()
    row_gh.x[1].start()
    row_gh.z.from_right()
    row_gh.x[3].start()
    ga_zl.start()
    row_gb.x[1].neighbours()
    row_gb.x[3].neighbours()
    row_gh.x[0].neighbours()
    row_gb.x[2].start()
    gt(token_block(x, 1), token_block(x, 3))
    row_gh.z.from_far()
    ga_zr.start()
    gt(token_block(xl, 0), token_block(xr, 0))
    ga_zl.neighbours()
    ga_x.from_far()
    ga_zf.start()
    row_up.x[2].neighbours()
    col_tok.far(0)
    col_tok.far(1)
    row_up.x[0].from_far()
    row_gb.x[0].from_far()
    ga_z.from_far()
    gt(token_block(x, 2))
    col_tok.paired()
    weights(x, early, True)
    weights(x, late)
    ga_zr.neighbours()
    row_gh.x[1].neighbours()
    gt(token_block(xl, 1), token_block(xr, 1))
    row_gh.x[3].neighbours()
    row_gh.x[2].start()
    gt(token_block(xl, 3), token_block(xr, 3))
    weights(xl, early)
    weights(xr, early)
    row_gh.x[0].from_far()
    gt(token_block(xf, 0))
    row_gb.x[2].neighbours()
    ga_zf.neighbours()
    for a in (row_up, row_gb):
        a.x[1].from_far()
        a.x[3].from_far()
    row_gh.x[1].from_far()
    gt(token_block(xf, 1))
    row_gh.x[2].neighbours()
    row_gh.x[3].from_far()
    gt(token_block(xf, 3))
    weights(xf, early)
    row_gh.x[2].rest()
    ga_zl.from_far()
    ga_zr.from_far()
    gt(token_block(xl, 2), token_block(xr, 2))
    for a in (row_up, row_gb):
        a.x[2].from_far()
    ga_zf.from_far()
    row_gh.x[2].from_far()
    last = token_block(xf, 2)
    gt_share(last)
    weights(xl, late)
    gt_finish(last)
    weights(xr, late)
    weights(xf, late)

    total = gt_acc[...]
    for m in range(1, 8):
        net.recv(block_rows(gt_r, m), m_gt + m)
        total = total + gt_r[pl.ds(m * B, B), :].astype(F32)
    gt_out[...] = total.astype(BF)

    net.drain()
    for q in range(8):
        net.copy(block_rows(d2d_s, q), block_rows(d2d_r, q), m_d2d + q, partner).wait_send()
    for m in range(1, 8):
        net.copy(block_rows(gt_s, m), block_rows(gt_r, m), m_gt + m, partner).wait_send()
    assert net.count <= N_MSG, net.count


def hand_over(*results):
    def body(*refs):
        copies = [pltpu.make_async_copy(src, dst, refs[8].at[i]) for i, (src, dst) in enumerate(zip(refs[:4], refs[4:8]))]
        for copy in copies:
            copy.start()
        for copy in copies:
            copy.wait()

    hbm = pl.BlockSpec(memory_space=pltpu.HBM)
    vmem = pl.BlockSpec(memory_space=pltpu.VMEM)
    return pl.pallas_call(
        body,
        name="hand_over",
        in_specs=[vmem] * 4,
        out_specs=(hbm,) * 4,
        out_shape=tuple(jax.ShapeDtypeStruct(a.shape, a.dtype) for a in results),
        scratch_shapes=[pltpu.SemaphoreType.DMA((4,))],
        compiler_params=pltpu.CompilerParams(vmem_limit_bytes=16 * 1024 * 1024),
    )(*results)


def per_device(tokens, grad_out, gate, up, gate_weight, up_weight, down_weight):
    f, d = gate.shape[1], tokens.shape[1]
    vmem = pl.BlockSpec(memory_space=pltpu.VMEM)
    hbm = pl.BlockSpec(memory_space=pltpu.HBM)
    results = pl.pallas_call(
        kernel,
        name="swiglu_backward",
        out_shape=(
            pltpu.VMEM((B, d), BF),
            pltpu.VMEM((d, f), F32),
            pltpu.VMEM((d, f), F32),
            pltpu.VMEM((d, f), F32),
        ),
        in_specs=[hbm] * 7,
        out_specs=(vmem,) * 4,
        scratch_shapes=[
            pltpu.VMEM((d, f), BF), pltpu.VMEM((d, f), BF), pltpu.VMEM((d, f), BF),
            pltpu.VMEM((16 * B, d), BF), pltpu.VMEM((16 * B, d), BF),
            pltpu.VMEM((f, d), BF), pltpu.VMEM((f, d), BF),
            pltpu.VMEM((16 * B, FIRST), BF), pltpu.VMEM((16 * B, f - FIRST), BF),
            pltpu.VMEM((16 * B, f), BF), pltpu.VMEM((16 * B, f), BF),
            pltpu.VMEM((16 * B, f), BF), pltpu.VMEM((16 * B, f), BF), pltpu.VMEM((16 * B, f), BF),
            pltpu.VMEM((16 * B, f), F32),
            pltpu.VMEM((4 * B, f), BF), pltpu.VMEM((4 * B, f), BF), pltpu.VMEM((4 * B, f), BF),
            pltpu.VMEM((4 * H, f), BF), pltpu.VMEM((4 * H, f), BF),
            pltpu.VMEM((4 * B, f), BF), pltpu.VMEM((4 * B, f), BF),
            pltpu.VMEM((B, f), F32),
            pltpu.VMEM((B, f), BF), pltpu.VMEM((B, f), BF), pltpu.VMEM((B, f), BF),
            pltpu.VMEM((H, f), BF), pltpu.VMEM((H, f), BF),
            pltpu.VMEM((B, f), BF), pltpu.VMEM((B, f), BF),
            pltpu.VMEM((8 * B, d), F32), pltpu.VMEM((8 * B, d), F32), pltpu.VMEM((8 * B, d), F32),
            pltpu.VMEM((8 * B, d), BF), pltpu.VMEM((8 * B, d), BF),
            pltpu.VMEM((B, d), F32),
            pltpu.SemaphoreType.DMA((N_MSG,)), pltpu.SemaphoreType.DMA((N_MSG,)), pltpu.SemaphoreType.DMA((8,)),
        ],
        compiler_params=pltpu.CompilerParams(
            collective_id=0, has_side_effects=True, vmem_limit_bytes=VMEM_LIMIT
        ),
    )(tokens, grad_out, gate, up, gate_weight, up_weight, down_weight)
    return hand_over(*results)


def solution(mesh):
    act, wide = P("col", "row"), P("row", "col")
    return jax.shard_map(
        per_device,
        mesh=mesh,
        in_specs=(act, act, wide, wide, wide, wide, wide),
        out_specs=(act, wide, wide, wide),
        check_vma=False,
    )
```

```python
import jax
import jax.numpy as jnp
from jax import lax
from jax.experimental import pallas as pl
from jax.experimental.pallas import tpu as pltpu
from jax.sharding import PartitionSpec as P

MESH = pl.DeviceIdType.MESH
BF = jnp.bfloat16
F32 = jnp.float32
B = 128
H = B // 2
N_MSG = 176
VMEM_LIMIT = 61_000_000
FIRST = 512


def rows(ref, start, size):
    return ref.at[pl.ds(pl.multiple_of(start, H), size), :]


class Net:
    def __init__(self, send, recv, me):
        self.send_sem, self.recv_sem, self.me = send, recv, me
        self.count = 0
        self.sent = []

    def take(self, n):
        first = self.count
        self.count += n
        return first

    def copy(self, src, dst, msg, device):
        return pltpu.make_async_remote_copy(
            src_ref=src, dst_ref=dst, send_sem=self.send_sem.at[msg], recv_sem=self.recv_sem.at[msg],
            device_id=device, device_id_type=MESH,
        )

    def send(self, src, dst, msg, device):
        copy = self.copy(src, dst, msg, device)
        copy.start()
        self.sent.append(copy)

    def recv(self, dst, msg):
        self.copy(dst, dst, msg, self.me).wait_recv()

    def drain(self):
        for copy in self.sent:
            copy.wait_send()


class Ring:
    def __init__(self, net, buf, pos, device_of, slot_of, split=False):
        self.net, self.buf, self.pos, self.device_of, self.slot_of = net, buf, pos, device_of, slot_of
        self.right, self.far, self.left = (lax.rem(pos + n, 4) for n in (1, 2, 3))
        self.split = split
        self.msg = net.take(6 if split else 4)

    def start(self):
        slot = self.slot_of(self.pos)
        first, second, own = rows(self.buf, slot, H), rows(self.buf, slot + H, H), rows(self.buf, slot, B)
        right, left = self.device_of(self.right), self.device_of(self.left)
        self.net.send(first if self.split else own, first if self.split else own, self.msg, right)
        self.net.send(second if self.split else own, second if self.split else own, self.msg + 1, left)
        if self.split:
            self.net.send(second, second, self.msg + 4, right)
            self.net.send(first, first, self.msg + 5, left)

    def from_left(self):
        slot = self.slot_of(self.left)
        half = rows(self.buf, slot, H)
        self.net.recv(half if self.split else rows(self.buf, slot, B), self.msg)
        self.net.send(half, half, self.msg + 2, self.device_of(self.right))

    def from_right(self):
        slot = self.slot_of(self.right)
        half = rows(self.buf, slot + H, H)
        self.net.recv(half if self.split else rows(self.buf, slot, B), self.msg + 1)
        self.net.send(half, half, self.msg + 3, self.device_of(self.left))

    def neighbours(self):
        self.from_left()
        self.from_right()

    def rest(self):
        self.net.recv(rows(self.buf, self.slot_of(self.left) + H, H), self.msg + 4)
        self.net.recv(rows(self.buf, self.slot_of(self.right), H), self.msg + 5)

    def from_far(self):
        slot = self.slot_of(self.far)
        self.net.recv(rows(self.buf, slot, H), self.msg + 2)
        self.net.recv(rows(self.buf, slot + H, H), self.msg + 3)


def dot(a, b, dims):
    return lax.dot_general(a, b, (dims, ((), ())), preferred_element_type=F32)


def kernel(
    tok_in, go_in, gate_in, up_in, gw_in, uw_in, dw_in,
    gt_out, dgw, duw, ddw,
    gw, uw, dw, go_all, tok_all, gwt, uwt, gate_a, gate_b, up, gh, hid, gg, gu, part, s1, s2r, s2l, r1l, r1r, r2l, r2r,
    xs, zs1, zs2r, zs2l, zr1l, zr1r, zr2l, zr2r,
    gt_own, d2d_s, d2d_r, gt_s, gt_r, gt_acc,
    send_sem, recv_sem, load_sem,
):
    row, col = lax.axis_index("row"), lax.axis_index("col")
    y, zl, k = lax.div(col, 4), lax.rem(lax.div(col, 2), 2), lax.rem(col, 2)

    def turned(p):
        return p + zl * (3 - 2 * p)

    x, zh = lax.div(row, 4), turned(lax.rem(row, 4))
    net = Net(send_sem, recv_sem, (row, col))
    other = 1 - zl

    def x_dev(p):
        return (p * 4 + turned(zh), col)

    def z_dev(p):
        return (x * 4 + turned(p), col)

    def y_dev(p):
        return (row, p * 4 + zl * 2 + k)

    partner = (row, y * 4 + zl * 2 + 1 - k)
    across = (row, y * 4 + other * 2 + k)
    xr, xf, xl = (lax.rem(x + n, 4) for n in (1, 2, 3))
    zr, zf, zlft = (lax.rem(zh + n, 4) for n in (1, 2, 3))

    barrier = pltpu.get_barrier_semaphore()
    peers = [x_dev(xr), x_dev(xl), z_dev(zr), z_dev(zlft), partner, across]
    for dy in (1, 2, 3):
        p = lax.rem(y + dy, 4)
        peers += [(row, p * 4 + zl * 2 + k), (row, p * 4 + other * 2 + k)]
    for peer in peers:
        pl.semaphore_signal(barrier, inc=1, device_id=peer, device_id_type=MESH)

    own = row * B
    sources = [
        (go_in, rows(go_all, col * B, B)),
        (up_in, rows(up, own, B)),
        (gate_in.at[:, pl.ds(FIRST, gate_in.shape[1] - FIRST)], rows(gate_b, own, B)),
        (gate_in.at[:, pl.ds(0, FIRST)], rows(gate_a, own, B)),
        (dw_in, dw),
        (tok_in, rows(tok_all, col * B, B)),
        (gw_in, gw),
        (uw_in, uw),
    ]
    loads = [pltpu.make_async_copy(src, dst, load_sem.at[i]) for i, (src, dst) in enumerate(sources)]
    for load in loads:
        load.start()
    pl.semaphore_wait(barrier, len(peers))

    class Column:
        def __init__(self, buf):
            self.buf = buf
            self.y0 = Ring(net, buf, y, y_dev, lambda p: (p * 4 + zl * 2 + k) * B)
            self.y1 = Ring(net, buf, y, y_dev, lambda p: (p * 4 + other * 2 + k) * B)
            self.m_across = net.take(1)
            self.m_pair = net.take(8)

        def slot(self, rel, flip, core):
            return (lax.rem(y + rel, 4) * 4 + (other if flip else zl) * 2 + core) * B

        def share(self, rel, flip):
            ref = rows(self.buf, self.slot(rel, flip, k), B)
            net.send(ref, ref, self.m_pair + rel * 2 + flip, partner)

        def start(self):
            mine = rows(self.buf, self.slot(0, 0, k), B)
            net.send(mine, mine, self.m_across, across)
            self.y0.start()
            self.share(0, 0)

        def crossed(self):
            net.recv(rows(self.buf, self.slot(0, 1, k), B), self.m_across)
            self.y1.start()
            self.share(0, 1)

        def near(self, flip):
            ring = self.y1 if flip else self.y0
            ring.from_left()
            self.share(3, flip)
            ring.from_right()
            self.share(1, flip)

        def far(self, flip):
            (self.y1 if flip else self.y0).from_far()
            self.share(2, flip)

        def paired(self):
            for rel in (0, 3, 1, 2):
                for flip in (0, 1):
                    net.recv(rows(self.buf, self.slot(rel, flip, 1 - k), B), self.m_pair + rel * 2 + flip)

    class Gather:
        def __init__(self, buf, split=()):
            self.z = Ring(net, buf, zh, z_dev, lambda p: (x * 4 + turned(p)) * B)
            self.x = {}
            for back in (0, 1, 3, 2):
                at = turned(lax.rem(zh + 4 - back, 4))
                self.x[back] = Ring(net, buf, x, x_dev, lambda p, at=at: (p * 4 + at) * B, back in split)

    col_go, col_tok = Column(go_all), Column(tok_all)
    row_up, row_gb, row_gh = Gather(up), Gather(gate_b), Gather(gh, (2,))
    ga_x = Ring(net, gate_a, x, x_dev, lambda p: (p * 4 + turned(zh)) * B)
    ga_z, ga_zl, ga_zr, ga_zf = (
        Ring(net, gate_a, zh, z_dev, lambda p, group=group: (group * 4 + turned(p)) * B) for group in (x, xl, xr, xf)
    )

    loads[0].wait()
    col_go.start()
    loads[1].wait()
    row_up.x[0].start()
    loads[2].wait()
    row_gb.x[0].start()
    loads[3].wait()
    ga_x.start()
    col_go.crossed()
    row_up.z.start()
    row_gb.z.start()
    col_go.near(0)
    row_up.x[0].neighbours()
    col_go.near(1)
    row_gb.x[0].neighbours()
    col_go.far(0)
    ga_x.neighbours()
    col_go.far(1)
    loads[4].wait()
    col_go.paired()

    nn = ((1,), (0,))

    def share_of(group):
        return dot(go_all[pl.ds(pl.multiple_of(group * 512, 512), 512), :], dw[...], nn)

    s1[...] = share_of(xf).astype(BF)
    order = (2, 1, 3, 0)
    dest = [turned(lax.rem(zh + off, 4)) for off in order]
    m1l, m1r, m2l, m2r = (net.take(4) for _ in range(4))
    for i, zb in enumerate(dest):
        net.send(rows(s1, zb * B, H), rows(r1l, i * H, H), m1l + i, x_dev(xr))
        net.send(rows(s1, zb * B + H, H), rows(r1r, i * H, H), m1r + i, x_dev(xl))
    for group in (xr, xl, x):
        part[pl.ds(pl.multiple_of(group * 512, 512), 512), :] = share_of(group)

    loads[5].wait()
    col_tok.start()
    row_up.z.neighbours()
    ga_z.start()
    for i, zb in enumerate(dest):
        lo, hi = pl.ds(i * B, H), pl.ds(i * B + H, H)
        base = (xr * 4 + zb) * B
        s2r[hi, :] = part[pl.ds(pl.multiple_of(base + H, H), H), :].astype(BF)
        net.recv(rows(r1l, i * H, H), m1l + i)
        s2r[lo, :] = (part[pl.ds(pl.multiple_of(base, H), H), :] + r1l[pl.ds(i * H, H), :].astype(F32)).astype(BF)
        net.send(rows(s2r, i * B, B), rows(r2l, i * B, B), m2l + i, x_dev(xr))
        base = (xl * 4 + zb) * B
        s2l[lo, :] = part[pl.ds(pl.multiple_of(base, H), H), :].astype(BF)
        net.recv(rows(r1r, i * H, H), m1r + i)
        s2l[hi, :] = (part[pl.ds(pl.multiple_of(base + H, H), H), :] + r1r[pl.ds(i * H, H), :].astype(F32)).astype(BF)
        net.send(rows(s2l, i * B, B), rows(r2r, i * B, B), m2r + i, x_dev(xl))
        if i == 1:
            row_gb.z.neighbours()
    col_tok.crossed()
    row_up.x[1].start()

    def x_sum(i):
        net.recv(rows(r2l, i * B, B), m2l + i)
        net.recv(rows(r2r, i * B, B), m2r + i)
        base = (x * 4 + dest[i]) * B
        at = pl.ds(i * B, B)
        return part[pl.ds(pl.multiple_of(base, B), B), :] + r2l[at, :].astype(F32) + r2r[at, :].astype(F32)

    mz = net.take(6)
    lo, hi = pl.ds(0, H), pl.ds(H, H)
    zs1[...] = x_sum(0).astype(BF)
    net.send(zs1.at[lo, :], zr1l, mz, z_dev(zr))
    net.send(zs1.at[hi, :], zr1r, mz + 1, z_dev(zlft))
    col_tok.near(0)
    row_up.x[3].start()
    loads[6].wait()
    loads[7].wait()
    gwt[...] = gw[...].T
    uwt[...] = uw[...].T
    xs[...] = x_sum(1)
    zs2r[hi, :] = xs[hi, :].astype(BF)
    net.send(zs2r.at[hi, :], zr2l.at[hi, :], mz + 2, z_dev(zr))
    net.recv(zr1l, mz)
    zs2r[lo, :] = (xs[lo, :] + zr1l[...].astype(F32)).astype(BF)
    net.send(zs2r.at[lo, :], zr2l.at[lo, :], mz + 3, z_dev(zr))
    xs[...] = x_sum(2)
    zs2l[lo, :] = xs[lo, :].astype(BF)
    net.send(zs2l.at[lo, :], zr2r.at[lo, :], mz + 4, z_dev(zlft))
    net.recv(zr1r, mz + 1)
    zs2l[hi, :] = (xs[hi, :] + zr1r[...].astype(F32)).astype(BF)
    net.send(zs2l.at[hi, :], zr2r.at[hi, :], mz + 5, z_dev(zlft))
    row_gb.x[1].start()
    row_gb.x[3].start()
    xs[...] = x_sum(3)
    net.recv(zr2l.at[hi, :], mz + 2)
    net.recv(zr2l.at[lo, :], mz + 3)
    net.recv(zr2r.at[lo, :], mz + 4)
    net.recv(zr2r.at[hi, :], mz + 5)

    gh[pl.ds(pl.multiple_of(own, B), B), :] = (xs[...] + zr2l[...].astype(F32) + zr2r[...].astype(F32)).astype(BF)
    row_gh.x[0].start()
    row_gh.z.start()
    ga_z.neighbours()
    col_tok.near(1)

    width = hid.shape[1]
    parts = ((gate_a, pl.ds(0, FIRST)), (gate_b, pl.ds(FIRST, width - FIRST)))

    def elementwise(j):
        def some(i, _):
            at = pl.ds(pl.multiple_of(j * B + i * 16, 16), 16)
            for gate, cols in parts:
                g, u, d = gate[at, :].astype(F32), up[at, cols].astype(F32), gh[at, cols].astype(F32)
                s = jax.nn.sigmoid(g)
                active = g * s
                hid[at, cols] = (active * u).astype(BF)
                gu[at, cols] = (d * active).astype(BF)
                gg[at, cols] = (d * u * s * (1.0 + g * (1.0 - s))).astype(BF)
            return 0

        lax.fori_loop(0, B // 16, some, 0)

    m_d2d, m_gt = net.take(8), net.take(8)

    def block_rows(ref, j):
        return rows(ref, j * B, B)

    def token_block(group, back):
        return group * 4 + turned(lax.rem(zh + 4 - back, 4))

    def gt_share(j):
        q = lax.div(j, 2)
        at = pl.ds(pl.multiple_of(j * B, B), B)
        here = pl.ds(pl.multiple_of(q * B, B), B)
        mine = lax.rem(j, 2) == k
        elementwise(j)
        value = dot(gg[at, :], gwt[...], nn) + dot(gu[at, :], uwt[...], nn)

        @pl.when(mine)
        def _():
            gt_own[here, :] = value

        @pl.when(jnp.logical_not(mine))
        def _():
            d2d_s[here, :] = value
            net.copy(block_rows(d2d_s, q), block_rows(d2d_r, q), m_d2d + q, partner).start()

    def gt_finish(j):
        q = lax.div(j, 2)
        here = pl.ds(pl.multiple_of(q * B, B), B)
        to_y, to_z = lax.div(j, 4), lax.rem(q, 2)
        m = lax.rem(to_y - y + 4, 4) * 2 + lax.rem(to_z - zl + 2, 2)

        @pl.when(lax.rem(j, 2) == k)
        def _():
            net.recv(block_rows(d2d_r, q), m_d2d + q)
            value = gt_own[here, :] + d2d_r[here, :]

            @pl.when(m == 0)
            def _():
                gt_acc[...] = value

            @pl.when(m != 0)
            def _():
                gt_s[pl.ds(pl.multiple_of(m * B, B), B), :] = value.astype(BF)
                net.copy(block_rows(gt_s, m), block_rows(gt_r, m), m_gt + m, (row, to_y * 4 + to_z * 2 + k)).start()

    waiting = []

    def flush():
        for j in waiting:
            gt_finish(j)
        waiting.clear()

    def gt(*blocks):
        for j in blocks:
            gt_share(j)
        flush()
        waiting.extend(blocks)

    tn = ((0,), (0,))

    early = lax.div(turned(zh), 2)
    late = 1 - early

    def weights(group, pair, first=False):
        at = pl.ds(pl.multiple_of(group * 512 + pair * 256, 256), 256)
        for out, left, right in ((dgw, tok_all, gg), (duw, tok_all, gu), (ddw, go_all, hid)):
            value = dot(left[at, :], right[at, :], tn)
            if first:
                out[...] = value
            else:
                out[...] += value

    gt(token_block(x, 0))
    row_up.x[1].neighbours()
    row_up.x[3].neighbours()
    row_up.z.from_far()
    row_gb.z.from_far()
    row_up.x[2].start()
    row_gh.z.from_left()
    row_gh.x[1].start()
    row_gh.z.from_right()
    row_gh.x[3].start()
    ga_zl.start()
    row_gb.x[1].neighbours()
    row_gb.x[3].neighbours()
    row_gh.x[0].neighbours()
    row_gb.x[2].start()
    gt(token_block(x, 1), token_block(x, 3))
    ga_zr.start()
    gt(token_block(xl, 0), token_block(xr, 0))
    row_up.x[2].neighbours()
    col_tok.far(0)
    col_tok.far(1)
    row_gh.z.from_far()
    ga_z.from_far()
    gt(token_block(x, 2))
    ga_x.from_far()
    ga_zl.neighbours()
    ga_zf.start()
    col_tok.paired()
    weights(x, early, True)
    weights(x, late)
    row_up.x[0].from_far()
    row_gb.x[0].from_far()
    row_gh.x[1].neighbours()
    row_gh.x[3].neighbours()
    row_gh.x[2].start()
    gt(token_block(xl, 1), token_block(xl, 3))
    weights(xl, early)
    ga_zr.neighbours()
    gt(token_block(xr, 1), token_block(xr, 3))
    weights(xr, early)
    row_gb.x[2].neighbours()
    row_gh.x[0].from_far()
    gt(token_block(xf, 0))
    ga_zf.neighbours()
    for a in (row_up, row_gb):
        a.x[1].from_far()
        a.x[3].from_far()
    row_gh.x[1].from_far()
    gt(token_block(xf, 1))
    flush()
    row_gh.x[2].neighbours()
    row_gh.x[3].from_far()
    gt(token_block(xf, 3))
    weights(xf, early)
    flush()
    row_gh.x[2].rest()
    ga_zl.from_far()
    ga_zr.from_far()
    gt(token_block(xl, 2), token_block(xr, 2))
    flush()
    for a in (row_up, row_gb):
        a.x[2].from_far()
    ga_zf.from_far()
    row_gh.x[2].from_far()
    last = token_block(xf, 2)
    gt_share(last)
    gt_finish(last)
    weights(xl, late)
    weights(xr, late)
    weights(xf, late)

    net.drain()
    for q in range(8):
        net.copy(block_rows(d2d_s, q), block_rows(d2d_r, q), m_d2d + q, partner).wait_send()
    for m in range(1, 8):
        net.copy(block_rows(gt_s, m), block_rows(gt_r, m), m_gt + m, partner).wait_send()

    total = gt_acc[...]
    for m in range(1, 8):
        net.recv(block_rows(gt_r, m), m_gt + m)
        total = total + gt_r[pl.ds(m * B, B), :].astype(F32)
    gt_out[...] = total.astype(BF)

    assert net.count <= N_MSG, net.count


def hand_over(*results):
    def body(*refs):
        copies = [pltpu.make_async_copy(src, dst, refs[8].at[i]) for i, (src, dst) in enumerate(zip(refs[:4], refs[4:8]))]
        for copy in copies:
            copy.start()
        for copy in copies:
            copy.wait()

    hbm = pl.BlockSpec(memory_space=pltpu.HBM)
    vmem = pl.BlockSpec(memory_space=pltpu.VMEM)
    return pl.pallas_call(
        body,
        name="hand_over",
        in_specs=[vmem] * 4,
        out_specs=(hbm,) * 4,
        out_shape=tuple(jax.ShapeDtypeStruct(a.shape, a.dtype) for a in results),
        scratch_shapes=[pltpu.SemaphoreType.DMA((4,))],
        compiler_params=pltpu.CompilerParams(vmem_limit_bytes=16 * 1024 * 1024),
    )(*results)


def per_device(tokens, grad_out, gate, up, gate_weight, up_weight, down_weight):
    f, d = gate.shape[1], tokens.shape[1]
    vmem = pl.BlockSpec(memory_space=pltpu.VMEM)
    hbm = pl.BlockSpec(memory_space=pltpu.HBM)
    results = pl.pallas_call(
        kernel,
        name="swiglu_backward",
        out_shape=(
            pltpu.VMEM((B, d), BF),
            pltpu.VMEM((d, f), F32),
            pltpu.VMEM((d, f), F32),
            pltpu.VMEM((d, f), F32),
        ),
        in_specs=[hbm] * 7,
        out_specs=(vmem,) * 4,
        scratch_shapes=[
            pltpu.VMEM((d, f), BF), pltpu.VMEM((d, f), BF), pltpu.VMEM((d, f), BF),
            pltpu.VMEM((16 * B, d), BF), pltpu.VMEM((16 * B, d), BF),
            pltpu.VMEM((f, d), BF), pltpu.VMEM((f, d), BF),
            pltpu.VMEM((16 * B, FIRST), BF), pltpu.VMEM((16 * B, f - FIRST), BF),
            pltpu.VMEM((16 * B, f), BF), pltpu.VMEM((16 * B, f), BF),
            pltpu.VMEM((16 * B, f), BF), pltpu.VMEM((16 * B, f), BF), pltpu.VMEM((16 * B, f), BF),
            pltpu.VMEM((16 * B, f), F32),
            pltpu.VMEM((4 * B, f), BF), pltpu.VMEM((4 * B, f), BF), pltpu.VMEM((4 * B, f), BF),
            pltpu.VMEM((4 * H, f), BF), pltpu.VMEM((4 * H, f), BF),
            pltpu.VMEM((4 * B, f), BF), pltpu.VMEM((4 * B, f), BF),
            pltpu.VMEM((B, f), F32),
            pltpu.VMEM((B, f), BF), pltpu.VMEM((B, f), BF), pltpu.VMEM((B, f), BF),
            pltpu.VMEM((H, f), BF), pltpu.VMEM((H, f), BF),
            pltpu.VMEM((B, f), BF), pltpu.VMEM((B, f), BF),
            pltpu.VMEM((8 * B, d), F32), pltpu.VMEM((8 * B, d), F32), pltpu.VMEM((8 * B, d), F32),
            pltpu.VMEM((8 * B, d), BF), pltpu.VMEM((8 * B, d), BF),
            pltpu.VMEM((B, d), F32),
            pltpu.SemaphoreType.DMA((N_MSG,)), pltpu.SemaphoreType.DMA((N_MSG,)), pltpu.SemaphoreType.DMA((8,)),
        ],
        compiler_params=pltpu.CompilerParams(
            collective_id=0, has_side_effects=True, vmem_limit_bytes=VMEM_LIMIT
        ),
    )(tokens, grad_out, gate, up, gate_weight, up_weight, down_weight)
    return hand_over(*results)


def solution(mesh):
    act, wide = P("col", "row"), P("row", "col")
    return jax.shard_map(
        per_device,
        mesh=mesh,
        in_specs=(act, act, wide, wide, wide, wide, wide),
        out_specs=(act, wide, wide, wide),
        check_vma=False,
    )
```

```python
import jax
import jax.numpy as jnp
from jax import lax
from jax.experimental import pallas as pl
from jax.experimental.pallas import tpu as pltpu
from jax.sharding import PartitionSpec as P

MESH = pl.DeviceIdType.MESH
BF = jnp.bfloat16
F32 = jnp.float32
B = 128
H = B // 2
N_MSG = 176
VMEM_LIMIT = 61_000_000
FIRST = 512


def rows(ref, start, size):
    return ref.at[pl.ds(pl.multiple_of(start, H), size), :]


class Net:
    def __init__(self, send, recv, me):
        self.send_sem, self.recv_sem, self.me = send, recv, me
        self.count = 0
        self.sent = []

    def take(self, n):
        first = self.count
        self.count += n
        return first

    def copy(self, src, dst, msg, device):
        return pltpu.make_async_remote_copy(
            src_ref=src, dst_ref=dst, send_sem=self.send_sem.at[msg], recv_sem=self.recv_sem.at[msg],
            device_id=device, device_id_type=MESH,
        )

    def send(self, src, dst, msg, device):
        copy = self.copy(src, dst, msg, device)
        copy.start()
        self.sent.append(copy)

    def recv(self, dst, msg):
        self.copy(dst, dst, msg, self.me).wait_recv()

    def drain(self):
        for copy in self.sent:
            copy.wait_send()


class Ring:
    def __init__(self, net, buf, pos, device_of, slot_of, split=False):
        self.net, self.buf, self.pos, self.device_of, self.slot_of = net, buf, pos, device_of, slot_of
        self.right, self.far, self.left = (lax.rem(pos + n, 4) for n in (1, 2, 3))
        self.split = split
        self.msg = net.take(6 if split else 4)

    def start(self):
        slot = self.slot_of(self.pos)
        first, second, own = rows(self.buf, slot, H), rows(self.buf, slot + H, H), rows(self.buf, slot, B)
        right, left = self.device_of(self.right), self.device_of(self.left)
        self.net.send(first if self.split else own, first if self.split else own, self.msg, right)
        self.net.send(second if self.split else own, second if self.split else own, self.msg + 1, left)
        if self.split:
            self.net.send(second, second, self.msg + 4, right)
            self.net.send(first, first, self.msg + 5, left)

    def from_left(self):
        slot = self.slot_of(self.left)
        half = rows(self.buf, slot, H)
        self.net.recv(half if self.split else rows(self.buf, slot, B), self.msg)
        self.net.send(half, half, self.msg + 2, self.device_of(self.right))

    def from_right(self):
        slot = self.slot_of(self.right)
        half = rows(self.buf, slot + H, H)
        self.net.recv(half if self.split else rows(self.buf, slot, B), self.msg + 1)
        self.net.send(half, half, self.msg + 3, self.device_of(self.left))

    def neighbours(self):
        self.from_left()
        self.from_right()

    def rest(self):
        self.net.recv(rows(self.buf, self.slot_of(self.left) + H, H), self.msg + 4)
        self.net.recv(rows(self.buf, self.slot_of(self.right), H), self.msg + 5)

    def from_far(self):
        slot = self.slot_of(self.far)
        self.net.recv(rows(self.buf, slot, H), self.msg + 2)
        self.net.recv(rows(self.buf, slot + H, H), self.msg + 3)


def dot(a, b, dims):
    return lax.dot_general(a, b, (dims, ((), ())), preferred_element_type=F32)


def kernel(
    tok_in, go_in, gate_in, up_in, gw_in, uw_in, dw_in,
    gt_out, dgw, duw, ddw,
    gw, uw, dw, go_all, tok_all, gwt, uwt, gate_a, gate_b, up, gh, hid, gg, gu, part, s1, s2r, s2l, r1l, r1r, r2l, r2r,
    xs, zs1, zs2r, zs2l, zr1l, zr1r, zr2l, zr2r,
    gt_own, d2d_s, d2d_r, gt_s, gt_r, gt_acc,
    send_sem, recv_sem, load_sem,
):
    row, col = lax.axis_index("row"), lax.axis_index("col")
    y, zl, k = lax.div(col, 4), lax.rem(lax.div(col, 2), 2), lax.rem(col, 2)

    def turned(p):
        return p + zl * (3 - 2 * p)

    x, zh = lax.div(row, 4), turned(lax.rem(row, 4))
    net = Net(send_sem, recv_sem, (row, col))
    other = 1 - zl

    def x_dev(p):
        return (p * 4 + turned(zh), col)

    def z_dev(p):
        return (x * 4 + turned(p), col)

    def y_dev(p):
        return (row, p * 4 + zl * 2 + k)

    partner = (row, y * 4 + zl * 2 + 1 - k)
    across = (row, y * 4 + other * 2 + k)
    xr, xf, xl = (lax.rem(x + n, 4) for n in (1, 2, 3))
    zr, zf, zlft = (lax.rem(zh + n, 4) for n in (1, 2, 3))

    barrier = pltpu.get_barrier_semaphore()
    peers = [x_dev(xr), x_dev(xl), z_dev(zr), z_dev(zlft), partner, across]
    for dy in (1, 2, 3):
        p = lax.rem(y + dy, 4)
        peers += [(row, p * 4 + zl * 2 + k), (row, p * 4 + other * 2 + k)]
    for peer in peers:
        pl.semaphore_signal(barrier, inc=1, device_id=peer, device_id_type=MESH)

    own = row * B
    sources = [
        (go_in, rows(go_all, col * B, B)),
        (up_in, rows(up, own, B)),
        (gate_in.at[:, pl.ds(FIRST, gate_in.shape[1] - FIRST)], rows(gate_b, own, B)),
        (gate_in.at[:, pl.ds(0, FIRST)], rows(gate_a, own, B)),
        (dw_in, dw),
        (tok_in, rows(tok_all, col * B, B)),
        (gw_in, gw),
        (uw_in, uw),
    ]
    loads = [pltpu.make_async_copy(src, dst, load_sem.at[i]) for i, (src, dst) in enumerate(sources)]
    for load in loads:
        load.start()
    pl.semaphore_wait(barrier, len(peers))

    class Column:
        def __init__(self, buf):
            self.buf = buf
            self.y0 = Ring(net, buf, y, y_dev, lambda p: (p * 4 + zl * 2 + k) * B)
            self.y1 = Ring(net, buf, y, y_dev, lambda p: (p * 4 + other * 2 + k) * B)
            self.m_across = net.take(1)
            self.m_pair = net.take(8)

        def slot(self, rel, flip, core):
            return (lax.rem(y + rel, 4) * 4 + (other if flip else zl) * 2 + core) * B

        def share(self, rel, flip):
            ref = rows(self.buf, self.slot(rel, flip, k), B)
            net.send(ref, ref, self.m_pair + rel * 2 + flip, partner)

        def start(self):
            mine = rows(self.buf, self.slot(0, 0, k), B)
            net.send(mine, mine, self.m_across, across)
            self.y0.start()
            self.share(0, 0)

        def crossed(self):
            net.recv(rows(self.buf, self.slot(0, 1, k), B), self.m_across)
            self.y1.start()
            self.share(0, 1)

        def near(self, flip):
            ring = self.y1 if flip else self.y0
            ring.from_left()
            self.share(3, flip)
            ring.from_right()
            self.share(1, flip)

        def far(self, flip):
            (self.y1 if flip else self.y0).from_far()
            self.share(2, flip)

        def paired(self):
            for rel in (0, 3, 1, 2):
                for flip in (0, 1):
                    net.recv(rows(self.buf, self.slot(rel, flip, 1 - k), B), self.m_pair + rel * 2 + flip)

    class Gather:
        def __init__(self, buf, split=()):
            self.z = Ring(net, buf, zh, z_dev, lambda p: (x * 4 + turned(p)) * B)
            self.x = {}
            for back in (0, 1, 3, 2):
                at = turned(lax.rem(zh + 4 - back, 4))
                self.x[back] = Ring(net, buf, x, x_dev, lambda p, at=at: (p * 4 + at) * B, back in split)

    col_go, col_tok = Column(go_all), Column(tok_all)
    row_up, row_gb, row_gh = Gather(up), Gather(gate_b), Gather(gh, (2,))
    ga_x = Ring(net, gate_a, x, x_dev, lambda p: (p * 4 + turned(zh)) * B)
    ga_z, ga_zl, ga_zr, ga_zf = (
        Ring(net, gate_a, zh, z_dev, lambda p, group=group: (group * 4 + turned(p)) * B) for group in (x, xl, xr, xf)
    )

    loads[0].wait()
    col_go.start()
    loads[1].wait()
    row_up.x[0].start()
    loads[2].wait()
    row_gb.x[0].start()
    loads[3].wait()
    ga_x.start()
    col_go.crossed()
    row_up.z.start()
    row_gb.z.start()
    col_go.near(0)
    row_up.x[0].neighbours()
    col_go.near(1)
    row_gb.x[0].neighbours()
    col_go.far(0)
    ga_x.neighbours()
    col_go.far(1)
    loads[4].wait()
    col_go.paired()

    nn = ((1,), (0,))

    def share_of(group):
        return dot(go_all[pl.ds(pl.multiple_of(group * 512, 512), 512), :], dw[...], nn)

    s1[...] = share_of(xf).astype(BF)
    order = (2, 1, 3, 0)
    dest = [turned(lax.rem(zh + off, 4)) for off in order]
    m1l, m1r, m2l, m2r = (net.take(4) for _ in range(4))
    for i, zb in enumerate(dest):
        net.send(rows(s1, zb * B, H), rows(r1l, i * H, H), m1l + i, x_dev(xr))
        net.send(rows(s1, zb * B + H, H), rows(r1r, i * H, H), m1r + i, x_dev(xl))
    for group in (xr, xl, x):
        part[pl.ds(pl.multiple_of(group * 512, 512), 512), :] = share_of(group)

    loads[5].wait()
    row_up.z.neighbours()
    ga_z.start()
    col_tok.start()
    for i, zb in enumerate(dest):
        lo, hi = pl.ds(i * B, H), pl.ds(i * B + H, H)
        base = (xr * 4 + zb) * B
        s2r[hi, :] = part[pl.ds(pl.multiple_of(base + H, H), H), :].astype(BF)
        net.recv(rows(r1l, i * H, H), m1l + i)
        s2r[lo, :] = (part[pl.ds(pl.multiple_of(base, H), H), :] + r1l[pl.ds(i * H, H), :].astype(F32)).astype(BF)
        net.send(rows(s2r, i * B, B), rows(r2l, i * B, B), m2l + i, x_dev(xr))
        base = (xl * 4 + zb) * B
        s2l[lo, :] = part[pl.ds(pl.multiple_of(base, H), H), :].astype(BF)
        net.recv(rows(r1r, i * H, H), m1r + i)
        s2l[hi, :] = (part[pl.ds(pl.multiple_of(base + H, H), H), :] + r1r[pl.ds(i * H, H), :].astype(F32)).astype(BF)
        net.send(rows(s2l, i * B, B), rows(r2r, i * B, B), m2r + i, x_dev(xl))
        if i == 1:
            row_gb.z.neighbours()
    row_up.x[1].start()

    def x_sum(i):
        net.recv(rows(r2l, i * B, B), m2l + i)
        net.recv(rows(r2r, i * B, B), m2r + i)
        base = (x * 4 + dest[i]) * B
        at = pl.ds(i * B, B)
        return part[pl.ds(pl.multiple_of(base, B), B), :] + r2l[at, :].astype(F32) + r2r[at, :].astype(F32)

    mz = net.take(6)
    lo, hi = pl.ds(0, H), pl.ds(H, H)
    zs1[...] = x_sum(0).astype(BF)
    net.send(zs1.at[lo, :], zr1l, mz, z_dev(zr))
    net.send(zs1.at[hi, :], zr1r, mz + 1, z_dev(zlft))
    row_up.x[3].start()
    col_tok.crossed()
    col_tok.near(0)
    loads[6].wait()
    loads[7].wait()
    gwt[...] = gw[...].T
    uwt[...] = uw[...].T
    xs[...] = x_sum(1)
    zs2r[hi, :] = xs[hi, :].astype(BF)
    net.send(zs2r.at[hi, :], zr2l.at[hi, :], mz + 2, z_dev(zr))
    net.recv(zr1l, mz)
    zs2r[lo, :] = (xs[lo, :] + zr1l[...].astype(F32)).astype(BF)
    net.send(zs2r.at[lo, :], zr2l.at[lo, :], mz + 3, z_dev(zr))
    xs[...] = x_sum(2)
    zs2l[lo, :] = xs[lo, :].astype(BF)
    net.send(zs2l.at[lo, :], zr2r.at[lo, :], mz + 4, z_dev(zlft))
    net.recv(zr1r, mz + 1)
    zs2l[hi, :] = (xs[hi, :] + zr1r[...].astype(F32)).astype(BF)
    net.send(zs2l.at[hi, :], zr2r.at[hi, :], mz + 5, z_dev(zlft))
    row_gb.x[1].start()
    row_gb.x[3].start()
    xs[...] = x_sum(3)
    net.recv(zr2l.at[hi, :], mz + 2)
    net.recv(zr2l.at[lo, :], mz + 3)
    net.recv(zr2r.at[lo, :], mz + 4)
    net.recv(zr2r.at[hi, :], mz + 5)

    gh[pl.ds(pl.multiple_of(own, B), B), :] = (xs[...] + zr2l[...].astype(F32) + zr2r[...].astype(F32)).astype(BF)
    row_gh.x[0].start()
    row_gh.z.start()
    ga_z.neighbours()
    col_tok.near(1)

    width = hid.shape[1]
    parts = ((gate_a, pl.ds(0, FIRST)), (gate_b, pl.ds(FIRST, width - FIRST)))

    def elementwise(j):
        def some(i, _):
            at = pl.ds(pl.multiple_of(j * B + i * 16, 16), 16)
            for gate, cols in parts:
                g, u, d = gate[at, :].astype(F32), up[at, cols].astype(F32), gh[at, cols].astype(F32)
                s = jax.nn.sigmoid(g)
                active = g * s
                hid[at, cols] = (active * u).astype(BF)
                gu[at, cols] = (d * active).astype(BF)
                gg[at, cols] = (d * u * s * (1.0 + g * (1.0 - s))).astype(BF)
            return 0

        lax.fori_loop(0, B // 16, some, 0)

    m_d2d, m_gt = net.take(8), net.take(8)

    def block_rows(ref, j):
        return rows(ref, j * B, B)

    def token_block(group, back):
        return group * 4 + turned(lax.rem(zh + 4 - back, 4))

    def gt_share(j):
        q = lax.div(j, 2)
        at = pl.ds(pl.multiple_of(j * B, B), B)
        here = pl.ds(pl.multiple_of(q * B, B), B)
        mine = lax.rem(j, 2) == k
        elementwise(j)
        value = dot(gg[at, :], gwt[...], nn) + dot(gu[at, :], uwt[...], nn)

        @pl.when(mine)
        def _():
            gt_own[here, :] = value

        @pl.when(jnp.logical_not(mine))
        def _():
            d2d_s[here, :] = value
            net.copy(block_rows(d2d_s, q), block_rows(d2d_r, q), m_d2d + q, partner).start()

    def gt_finish(j):
        q = lax.div(j, 2)
        here = pl.ds(pl.multiple_of(q * B, B), B)
        to_y, to_z = lax.div(j, 4), lax.rem(q, 2)
        m = lax.rem(to_y - y + 4, 4) * 2 + lax.rem(to_z - zl + 2, 2)

        @pl.when(lax.rem(j, 2) == k)
        def _():
            net.recv(block_rows(d2d_r, q), m_d2d + q)
            value = gt_own[here, :] + d2d_r[here, :]

            @pl.when(m == 0)
            def _():
                gt_acc[...] = value

            @pl.when(m != 0)
            def _():
                gt_s[pl.ds(pl.multiple_of(m * B, B), B), :] = value.astype(BF)
                net.copy(block_rows(gt_s, m), block_rows(gt_r, m), m_gt + m, (row, to_y * 4 + to_z * 2 + k)).start()

    waiting = []

    def flush():
        for j in waiting:
            gt_finish(j)
        waiting.clear()

    def gt(*blocks):
        for j in blocks:
            gt_share(j)
        flush()
        waiting.extend(blocks)

    tn = ((0,), (0,))

    early = lax.div(turned(zh), 2)
    late = 1 - early

    def weights(group, pair, first=False):
        at = pl.ds(pl.multiple_of(group * 512 + pair * 256, 256), 256)
        for out, left, right in ((dgw, tok_all, gg), (duw, tok_all, gu), (ddw, go_all, hid)):
            value = dot(left[at, :], right[at, :], tn)
            if first:
                out[...] = value
            else:
                out[...] += value

    gt(token_block(x, 0))
    row_up.x[1].neighbours()
    row_up.x[3].neighbours()
    row_up.z.from_far()
    row_gb.z.from_far()
    row_up.x[2].start()
    row_gh.z.from_left()
    row_gh.x[1].start()
    row_gh.z.from_right()
    row_gh.x[3].start()
    ga_zl.start()
    row_gb.x[1].neighbours()
    row_gb.x[3].neighbours()
    row_gh.x[0].neighbours()
    row_gb.x[2].start()
    gt(token_block(x, 1), token_block(x, 3))
    ga_zr.start()
    gt(token_block(xl, 0), token_block(xr, 0))
    row_up.x[2].neighbours()
    col_tok.far(0)
    col_tok.far(1)
    row_gh.z.from_far()
    ga_z.from_far()
    gt(token_block(x, 2))
    ga_x.from_far()
    ga_zl.neighbours()
    ga_zf.start()
    col_tok.paired()
    weights(x, early, True)
    weights(x, late)
    row_up.x[0].from_far()
    row_gb.x[0].from_far()
    row_gh.x[1].neighbours()
    row_gh.x[3].neighbours()
    row_gh.x[2].start()
    gt(token_block(xl, 1), token_block(xl, 3))
    weights(xl, early)
    ga_zr.neighbours()
    gt(token_block(xr, 1), token_block(xr, 3))
    weights(xr, early)
    row_gb.x[2].neighbours()
    row_gh.x[0].from_far()
    gt(token_block(xf, 0))
    ga_zf.neighbours()
    for a in (row_up, row_gb):
        a.x[1].from_far()
        a.x[3].from_far()
    row_gh.x[1].from_far()
    gt(token_block(xf, 1))
    flush()
    row_gh.x[2].neighbours()
    row_gh.x[3].from_far()
    gt(token_block(xf, 3))
    weights(xf, early)
    flush()
    row_gh.x[2].rest()
    ga_zl.from_far()
    ga_zr.from_far()
    gt(token_block(xl, 2), token_block(xr, 2))
    flush()
    for a in (row_up, row_gb):
        a.x[2].from_far()
    ga_zf.from_far()
    row_gh.x[2].from_far()
    last = token_block(xf, 2)
    gt_share(last)
    gt_finish(last)
    weights(xl, late)
    weights(xr, late)
    weights(xf, late)

    net.drain()
    for q in range(8):
        net.copy(block_rows(d2d_s, q), block_rows(d2d_r, q), m_d2d + q, partner).wait_send()
    for m in range(1, 8):
        net.copy(block_rows(gt_s, m), block_rows(gt_r, m), m_gt + m, partner).wait_send()

    total = gt_acc[...]
    for m in range(1, 8):
        net.recv(block_rows(gt_r, m), m_gt + m)
        total = total + gt_r[pl.ds(m * B, B), :].astype(F32)
    gt_out[...] = total.astype(BF)

    assert net.count <= N_MSG, net.count


def hand_over(*results):
    def body(*refs):
        copies = [pltpu.make_async_copy(src, dst, refs[8].at[i]) for i, (src, dst) in enumerate(zip(refs[:4], refs[4:8]))]
        for copy in copies:
            copy.start()
        for copy in copies:
            copy.wait()

    hbm = pl.BlockSpec(memory_space=pltpu.HBM)
    vmem = pl.BlockSpec(memory_space=pltpu.VMEM)
    return pl.pallas_call(
        body,
        name="hand_over",
        in_specs=[vmem] * 4,
        out_specs=(hbm,) * 4,
        out_shape=tuple(jax.ShapeDtypeStruct(a.shape, a.dtype) for a in results),
        scratch_shapes=[pltpu.SemaphoreType.DMA((4,))],
        compiler_params=pltpu.CompilerParams(vmem_limit_bytes=16 * 1024 * 1024),
    )(*results)


def per_device(tokens, grad_out, gate, up, gate_weight, up_weight, down_weight):
    f, d = gate.shape[1], tokens.shape[1]
    vmem = pl.BlockSpec(memory_space=pltpu.VMEM)
    hbm = pl.BlockSpec(memory_space=pltpu.HBM)
    results = pl.pallas_call(
        kernel,
        name="swiglu_backward",
        out_shape=(
            pltpu.VMEM((B, d), BF),
            pltpu.VMEM((d, f), F32),
            pltpu.VMEM((d, f), F32),
            pltpu.VMEM((d, f), F32),
        ),
        in_specs=[hbm] * 7,
        out_specs=(vmem,) * 4,
        scratch_shapes=[
            pltpu.VMEM((d, f), BF), pltpu.VMEM((d, f), BF), pltpu.VMEM((d, f), BF),
            pltpu.VMEM((16 * B, d), BF), pltpu.VMEM((16 * B, d), BF),
            pltpu.VMEM((f, d), BF), pltpu.VMEM((f, d), BF),
            pltpu.VMEM((16 * B, FIRST), BF), pltpu.VMEM((16 * B, f - FIRST), BF),
            pltpu.VMEM((16 * B, f), BF), pltpu.VMEM((16 * B, f), BF),
            pltpu.VMEM((16 * B, f), BF), pltpu.VMEM((16 * B, f), BF), pltpu.VMEM((16 * B, f), BF),
            pltpu.VMEM((16 * B, f), F32),
            pltpu.VMEM((4 * B, f), BF), pltpu.VMEM((4 * B, f), BF), pltpu.VMEM((4 * B, f), BF),
            pltpu.VMEM((4 * H, f), BF), pltpu.VMEM((4 * H, f), BF),
            pltpu.VMEM((4 * B, f), BF), pltpu.VMEM((4 * B, f), BF),
            pltpu.VMEM((B, f), F32),
            pltpu.VMEM((B, f), BF), pltpu.VMEM((B, f), BF), pltpu.VMEM((B, f), BF),
            pltpu.VMEM((H, f), BF), pltpu.VMEM((H, f), BF),
            pltpu.VMEM((B, f), BF), pltpu.VMEM((B, f), BF),
            pltpu.VMEM((8 * B, d), F32), pltpu.VMEM((8 * B, d), F32), pltpu.VMEM((8 * B, d), F32),
            pltpu.VMEM((8 * B, d), BF), pltpu.VMEM((8 * B, d), BF),
            pltpu.VMEM((B, d), F32),
            pltpu.SemaphoreType.DMA((N_MSG,)), pltpu.SemaphoreType.DMA((N_MSG,)), pltpu.SemaphoreType.DMA((8,)),
        ],
        compiler_params=pltpu.CompilerParams(
            collective_id=0, has_side_effects=True, vmem_limit_bytes=VMEM_LIMIT
        ),
    )(tokens, grad_out, gate, up, gate_weight, up_weight, down_weight)
    return hand_over(*results)


def solution(mesh):
    act, wide = P("col", "row"), P("row", "col")
    return jax.shard_map(
        per_device,
        mesh=mesh,
        in_specs=(act, act, wide, wide, wide, wide, wide),
        out_specs=(act, wide, wide, wide),
        check_vma=False,
    )
```
